32 devices in a mesh: dp: 8 (over y, x, core), tm: 4 (over z).
Axes of the slice: x: 2, y: 2, z: 4, core: 2. Of those that a mesh axis runs over, the one named last changes fastest.
Arguments:
- audio: float32 [24, 8, 1024], P('dp', None, 'tm'), may hold values from -3.15 to 3.15, as said below
- mel_frames: bfloat16 [24, 1024, 640], P('dp', 'tm'), may hold values from -6 to 6
- start_weight: float32 [4, 512], replicated, may hold values from -3 to 3
- input_weight: bfloat16 [2, 3, 512, 1024], replicated, may hold values from -0.15625 to 0.15625
- cond_weight: bfloat16 [2, 640, 1024], replicated, may hold values from -0.25 to 0.25
- res_weight: bfloat16 [1, 512, 1024], replicated, may hold values from -0.25 to 0.25
- last_weight: bfloat16 [512, 512], replicated, may hold values from -0.25 to 0.25
- end_weight: bfloat16 [512, 8], replicated, may hold values from -0.25 to 0.25
Outputs:
- latent: float32 [24, 4, 1024], P('dp', None, 'tm')
- audio_grad: float32 [24, 8, 1024], P('dp', None, 'tm')
- batch_loss: float32 [], replicated
- input_weight_grad: float32 [2, 3, 512, 1024], P(None, None, 'dp', 'tm')
- cond_weight_grad: float32 [2, 640, 1024], P(None, 'dp', 'tm')
- res_weight_grad: float32 [1, 512, 1024], P(None, 'dp', 'tm')
- last_weight_grad: float32 [512, 512], replicated
- end_weight_grad: float32 [512, 8], replicated
- start_weight_grad: float32 [4, 512], replicated
The draws below stay inside these ranges and needn't reach their ends.
Inputs may be any that keep to these rules, and one draw needn't show every extreme that they name: `audio`: audio samples.
All inputs are finite; a program needn't handle non-finite values.
Results may differ from the reference program's by a relative error of at most 0.015.
Values may be sent and summed in bfloat16 or wider, within the bound.
A program may use at most 128 MiB of HBM per device.

```python
import jax
import jax.numpy as jnp
from jax import lax

C = 512
COND = 640
GROUP = 8
TAPS = 3
LAYERS = 2
HALF = 4
CLIPS = 24
FRAMES = 1024


def draw_audio(key, part):
    first_key = jax.random.fold_in(key, 0)
    clip_rise = 1.0 + 2.0 * jnp.arange(CLIPS, dtype=jnp.float32) / max(CLIPS - 1, 1)
    time_rise = 1.0 + 2.0 * jnp.arange(FRAMES, dtype=jnp.float32) / max(FRAMES - 1, 1)
    envelope = clip_rise[:, None, None] * time_rise[None, None, :]
    values = 0.1 * jnp.clip(jax.random.normal(first_key, (CLIPS, GROUP, FRAMES), jnp.float32), -3.5, 3.5)
    return values * envelope


def steps_of(rng, shape, shards, low, top_value):
    factor_of = 1.0
    for axis_at, parts in shards:
        steps = jax.random.uniform(jax.random.fold_in(jax.random.fold_in(rng, 6), axis_at), (parts,), jnp.float32, low / len(shards), top_value / len(shards))
        factor_of = factor_of * jnp.repeat(jnp.exp(steps), shape[axis_at] // parts).reshape((-1,) + (1,) * (len(shape) - 1 - axis_at))
    return factor_of


def gaussian(key, dims, scale, most, cuts=(), held_as=jnp.bfloat16):
    level = steps_of(key, dims, cuts, -0.22, 0.18) if cuts else 1.0
    drawn = jax.random.normal(key, dims, jnp.float32) * scale * level
    return jnp.minimum(jnp.maximum(drawn, -most), most).astype(held_as)


def setup_inputs(seed: int = 0) -> dict:
    seeds = jax.random.split(jax.random.key(seed), 9)
    audio = draw_audio(jax.random.fold_in(seeds[8], 71), 0)
    mel_frames = gaussian(seeds[1], (CLIPS, FRAMES, COND), 1.0, 6.0, ((0, 8), (1, 4)))
    start_weight = gaussian(seeds[2], (HALF, C), HALF ** -0.5, 3.0, (), jnp.float32)
    input_weight = gaussian(seeds[3], (LAYERS, TAPS, C, 2 * C), (TAPS * C) ** -0.5, 0.15625)
    cond_weight = gaussian(seeds[4], (LAYERS, COND, 2 * C), COND ** -0.5, 0.25)
    res_weight = gaussian(seeds[5], (LAYERS - 1, C, 2 * C), C ** -0.5, 0.25)
    last_weight = gaussian(seeds[6], (C, C), C ** -0.5, 0.25)
    end_weight = gaussian(seeds[7], (C, GROUP), C ** -0.5, 0.25)
    return {"audio": audio, "mel_frames": mel_frames, "start_weight": start_weight, "input_weight": input_weight, "cond_weight": cond_weight, "res_weight": res_weight, "last_weight": last_weight, "end_weight": end_weight}


highest = lax.Precision.HIGHEST


def gated_unit(pre_act, channels):
    return jnp.tanh(pre_act[:, :channels]) * jax.nn.sigmoid(pre_act[:, channels:])


def gated_back(pre_act, upstream, channels):
    tangent = jnp.tanh(pre_act[:, :channels])
    switch = jax.nn.sigmoid(pre_act[:, channels:])
    return jnp.concatenate([upstream * (1.0 - tangent * tangent) * switch, upstream * tangent * switch * (1.0 - switch)], axis=1)


def dilated(padded, weight, spread, length):
    summed = jnp.zeros((length, weight.shape[2]), jnp.float32)
    for tap_index in range(weight.shape[0]):
        window = padded[tap_index * spread:tap_index * spread + length]
        summed = summed + jnp.dot(window, weight[tap_index], preferred_element_type=jnp.float32)
    return summed


def dilated_back(padded_grad, weight, spread, length):
    taps = weight.shape[0]
    summed = jnp.zeros((length, weight.shape[1]), jnp.float32)
    for tap_index in range(taps):
        offset = (taps - 1 - tap_index) * spread
        window = padded_grad[offset:offset + length]
        summed = summed + jnp.dot(window, weight[tap_index].T, preferred_element_type=jnp.float32)
    return summed


def clip_work(audio_clip, mel_clip, weights, scale_inv):
    start_weight, input_weight, cond_weight, res_weight, last_weight, end_weight = weights
    half_group = audio_clip.shape[0] // 2
    length = audio_clip.shape[1]
    channels = start_weight.shape[1]
    taps = input_weight.shape[1]
    first_half = audio_clip[:half_group].T
    second_half = audio_clip[half_group:].T
    hidden = jnp.dot(first_half, start_weight, precision=highest)
    skip_sum = jnp.zeros((length, channels), jnp.float32)
    stored = []
    for layer_index in range(LAYERS):
        spread = 2 ** layer_index
        state_b = hidden.astype(jnp.bfloat16)
        padded = jnp.pad(state_b, ((spread, spread), (0, 0)))
        pre_act = dilated(padded, input_weight[layer_index], spread, length) + jnp.dot(mel_clip, cond_weight[layer_index], preferred_element_type=jnp.float32)
        gated_out = gated_unit(pre_act, channels).astype(jnp.bfloat16)
        stored.append((padded, pre_act, gated_out))
        if layer_index < LAYERS - 1:
            mixed = jnp.dot(gated_out, res_weight[layer_index], preferred_element_type=jnp.float32)
            hidden = hidden + mixed[:, :channels]
            skip_sum = skip_sum + mixed[:, channels:]
        else:
            skip_sum = skip_sum + jnp.dot(gated_out, last_weight, preferred_element_type=jnp.float32)
    skip_b = skip_sum.astype(jnp.bfloat16)
    outputs = jnp.dot(skip_b, end_weight, preferred_element_type=jnp.float32)
    log_scale = outputs[:, :half_group]
    shift_term = outputs[:, half_group:]
    growth = jnp.exp(log_scale)
    latent_rows = growth * second_half + shift_term
    loss_part = (0.5 * jnp.sum(first_half * first_half) + 0.5 * jnp.sum(latent_rows * latent_rows) - jnp.sum(log_scale)) * scale_inv
    grad_out = jnp.concatenate([(latent_rows * growth * second_half - 1.0) * scale_inv, latent_rows * scale_inv], axis=1).astype(jnp.bfloat16)
    end_grad = jnp.dot(skip_b.T, grad_out, preferred_element_type=jnp.float32)
    skip_back = jnp.dot(grad_out, end_weight.T, preferred_element_type=jnp.float32).astype(jnp.bfloat16)
    state_back = jnp.zeros((length, channels), jnp.float32)
    in_grads = [None] * LAYERS
    cond_grads = [None] * LAYERS
    res_grads = [None] * (LAYERS - 1)
    last_grad = None
    for layer_index in reversed(range(LAYERS)):
        spread = 2 ** layer_index
        padded, pre_act, gated_out = stored[layer_index]
        if layer_index == LAYERS - 1:
            act_back = jnp.dot(skip_back, last_weight.T, preferred_element_type=jnp.float32)
            last_grad = jnp.dot(gated_out.T, skip_back, preferred_element_type=jnp.float32)
        else:
            joined = jnp.concatenate([state_back.astype(jnp.bfloat16), skip_back], axis=1)
            act_back = jnp.dot(joined, res_weight[layer_index].T, preferred_element_type=jnp.float32)
            res_grads[layer_index] = jnp.dot(gated_out.T, joined, preferred_element_type=jnp.float32)
        pre_back = gated_back(pre_act, act_back, channels).astype(jnp.bfloat16)
        in_grads[layer_index] = jnp.stack([jnp.dot(padded[tap_index * spread:tap_index * spread + length].T, pre_back, preferred_element_type=jnp.float32) for tap_index in range(taps)])
        cond_grads[layer_index] = jnp.dot(mel_clip.T, pre_back, preferred_element_type=jnp.float32)
        grad_pad = jnp.pad(pre_back, ((spread, spread), (0, 0)))
        state_back = state_back + dilated_back(grad_pad, input_weight[layer_index], spread, length)
    start_grad = jnp.dot(first_half.T, state_back, precision=highest)
    first_back = jnp.dot(state_back, start_weight.T, precision=highest) + first_half * scale_inv
    audio_back = jnp.concatenate([first_back, latent_rows * growth * scale_inv], axis=1).T
    grads = (jnp.stack(in_grads), jnp.stack(cond_grads), jnp.stack(res_grads), last_grad, end_grad, start_grad)
    return latent_rows.T, audio_back, loss_part, grads


def reference(audio, mel_frames, start_weight, input_weight, cond_weight, res_weight, last_weight, end_weight):
    weights = (start_weight, input_weight, cond_weight, res_weight, last_weight, end_weight)
    scale_inv = 1.0 / CLIPS
    channels = start_weight.shape[1]
    initial = (jnp.zeros((), jnp.float32),
               jnp.zeros(input_weight.shape, jnp.float32),
               jnp.zeros(cond_weight.shape, jnp.float32),
               jnp.zeros(res_weight.shape, jnp.float32),
               jnp.zeros((channels, channels), jnp.float32),
               jnp.zeros(end_weight.shape, jnp.float32),
               jnp.zeros(start_weight.shape, jnp.float32))

    def clip_step(running, clip_pair):
        audio_clip, mel_clip = clip_pair
        latent_clip, audio_back, loss_part, grads = clip_work(audio_clip, mel_clip, weights, scale_inv)
        running = jax.tree.map(lambda held, current: held + current, running, (loss_part,) + grads)
        return running, (latent_clip, audio_back)

    summed_all, stacked = lax.scan(clip_step, initial, (audio, mel_frames))
    batch_loss, in_grad, cond_grad, res_grad, last_grad, end_grad, start_grad = summed_all
    return stacked[0], stacked[1], batch_loss, in_grad, cond_grad, res_grad, last_grad, end_grad, start_grad
```

```python
import itertools

import jax
import jax.numpy as jnp
from jax import lax
from jax.experimental import pallas as pl
from jax.experimental.pallas import tpu as pltpu
from jax.sharding import PartitionSpec as P

F32 = jnp.float32
BF16 = jnp.bfloat16
HIGHEST = lax.Precision.HIGHEST
MESH = pl.DeviceIdType.MESH
EDGE = 8
BLOCK = 256
LANES = 128


def dot(a, b, dims=((1,), (0,)), precision=None):
    return lax.dot_general(
        a, b, (dims, ((), ())), precision=precision, preferred_element_type=F32
    )


def round_up(value, unit):
    return -(-value // unit) * unit


class Plan:
    def __init__(self, mesh, audio, mel, start_weight, input_weight):
        self.dp, self.tm = mesh.shape["dp"], mesh.shape["tm"]
        self.bits = self.dp.bit_length() - 1
        self.clips, self.group, self.frames = audio.shape
        self.half = self.group // 2
        self.cond = mel.shape[2]
        self.channels = start_weight.shape[1]
        self.layers, self.taps = input_weight.shape[:2]
        self.wide = 2 * self.channels
        self.rows = self.clips * self.frames
        self.all_rows = self.rows + self.clips * 2 * EDGE
        self.pad_rows = round_up(self.all_rows, LANES)
        self.own_ch = self.channels // self.dp
        self.own_cond = self.cond // self.dp
        self.width = self.wide // self.tm
        order = list(range(self.bits))
        self.first = order
        self.second = order[:1] + order[1:][::-1]
        tap_pair = tuple(range(self.taps - 1))
        rest = (self.taps - 1, "cond")
        self.chunks = [
            (1, tap_pair, self.wide, self.first),
            (1, rest, self.wide, self.second),
            (0, ("res",), self.channels, self.second),
            (0, tap_pair, self.wide, self.first),
            (0, rest, self.wide, self.second),
        ]

    def part_rows(self, part):
        return self.own_cond if part == "cond" else self.own_ch

    def chunk_rows(self, chunk):
        return round_up(sum(self.part_rows(part) for part in chunk[1]), 16)


def kernel(plan, *refs):
    p = plan
    n_in, n_out = 8, 9
    (audio_h, mel_h, start_w, win_h, cond_h, res_h, last_h, end_w) = refs[:n_in]
    (
        latent_o, audio_o, loss_o, in_o, cond_o, res_o, last_o, end_o, start_o
    ) = refs[n_in : n_in + n_out]
    s = refs[n_in + n_out]
    me_dp, me_tm = lax.axis_index("dp"), lax.axis_index("tm")
    bit_of = [(me_dp // 2**b) % 2 for b in range(p.bits)]
    ch, rows, all_rows, fr = p.channels, p.rows, p.all_rows, p.frames
    ext = fr + 2 * EDGE
    n_blocks = ch // BLOCK

    def partner(b):
        return {"dp": me_dp + (2**b) * (1 - 2 * bit_of[b]), "tm": me_tm}

    def peer(step):
        return {"dp": me_dp, "tm": lax.rem(me_tm + step, p.tm)}

    loads = {}

    def load(name, src, dst, index):
        copy = pltpu.make_async_copy(src, dst, s["load_sem"].at[index])
        copy.start()
        loads[name] = copy

    load("audio", audio_h, s["audio"], 0)
    for clip in range(p.clips):
        load(
            f"mel{clip}", mel_h.at[clip], s["mel"].at[pl.ds(clip * fr, fr)], 1 + clip
        )
    base = 1 + p.clips
    for layer in range(p.layers):
        load(f"win{layer}", win_h.at[layer], s["win"].at[layer], base + 2 * layer)
        load(f"cond{layer}", cond_h.at[layer], s["cond"].at[layer], base + 2 * layer + 1)
        if layer == 0:
            load("res", res_h, s["res"], base + 2 * p.layers)
            load("last", last_h, s["last"], base + 2 * p.layers + 1)

    barrier = pltpu.get_barrier_semaphore()
    for b in range(p.bits):
        pl.semaphore_signal(barrier, 1, device_id=partner(b), device_id_type=MESH)
    for step in range(1, p.tm):
        pl.semaphore_signal(barrier, 1, device_id=peer(step), device_id_type=MESH)
    pl.semaphore_wait(barrier, p.bits + p.tm - 1)

    has_low, has_high = me_tm > 0, me_tm < p.tm - 1

    def halo_copies(slot):
        device = {"dp": me_dp, "tm": me_tm + 1 if slot == 0 else me_tm - 1}
        mel_at = fr - 2 * EDGE if slot == 0 else 0
        audio_at = fr - LANES if slot == 0 else 0
        return [
            pltpu.make_async_remote_copy(
                audio_h.at[:, :, pl.ds(audio_at, LANES)],
                s["audio_halo"].at[slot],
                s["halo_send"].at[slot, 0], s["halo_recv"].at[slot, 0],
                device_id=device, device_id_type=MESH,
            ),
            pltpu.make_async_remote_copy(
                mel_h.at[:, pl.ds(mel_at, 2 * EDGE)],
                s["mel_halo"].at[slot],
                s["halo_send"].at[slot, 1], s["halo_recv"].at[slot, 1],
                device_id=device, device_id_type=MESH,
            ),
        ]

    to_high, to_low = halo_copies(0), halo_copies(1)

    @pl.when(has_high)
    def _():
        for copy in to_high:
            copy.start()

    @pl.when(has_low)
    def _():
        for copy in to_low:
            copy.start()

    def halo_wait(index):
        @pl.when(has_low)
        def _():
            to_high[index].wait_recv()

        @pl.when(has_high)
        def _():
            to_low[index].wait_recv()

    def free_bits(order, stage):
        done = set(order[:stage])
        return [b for b in reversed(range(p.bits)) if b not in done]

    def g_index(values):
        return tuple(values[b] for b in reversed(range(p.bits)))

    def g_blocks(chunk_id, stage, other):
        order = p.chunks[chunk_id][3]
        bit = order[stage]
        free = free_bits(order, stage + 1)
        for combo in itertools.product((0, 1), repeat=len(free)):
            values = {b: bit_of[b] for b in order[:stage]}
            values[bit] = 1 - bit_of[bit] if other else bit_of[bit]
            values.update(zip(free, combo))
            yield values

    def recv_index(order, stage, values):
        return tuple(values[b] for b in free_bits(order, stage + 1))

    def add_block(chunk_id, stages, values):
        order = p.chunks[chunk_id][3]
        acc = s["grad"][chunk_id]
        at = g_index(values)
        height = acc.shape[-2]

        @pl.loop(0, height // 16)
        def _(r):
            where = (pl.ds(pl.multiple_of(r * 16, 16), 16),)
            total = acc[at + where].astype(F32)
            for stage in range(stages):
                buf = s["recv"][chunk_id][stage]
                total += buf[recv_index(order, stage, values) + where].astype(F32)
            acc[at + where] = total.astype(BF16)

    def stage_copy(chunk_id, stage):
        order = p.chunks[chunk_id][3]
        bit = order[stage]
        values = {b: slice(None) for b in range(p.bits)}
        values.update({b: bit_of[b] for b in order[:stage]})
        values[bit] = 1 - bit_of[bit]
        return pltpu.make_async_remote_copy(
            s["grad"][chunk_id].at[g_index(values)],
            s["recv"][chunk_id][stage],
            s["dp_send"].at[chunk_id, stage], s["dp_recv"].at[chunk_id, stage],
            device_id=partner(bit), device_id_type=MESH,
        )

    def dp_send(chunk_id, stage):
        if stage:
            stage_copy(chunk_id, stage - 1).wait_recv()
            for values in g_blocks(chunk_id, stage, True):
                add_block(chunk_id, stage, values)
        stage_copy(chunk_id, stage).start()

    def owners(chunk_id):
        return p.chunks[chunk_id][2] // p.width

    def tm_copy(chunk_id, step):
        target = lax.rem(me_tm + step, p.tm)
        at = g_index({b: bit_of[b] for b in range(p.bits)})
        place = lax.rem(target, owners(chunk_id))
        cols = pl.ds(pl.multiple_of(place * p.width, LANES), p.width)
        return pltpu.make_async_remote_copy(
            s["grad"][chunk_id].at[at + (slice(None), cols)],
            s["tm_recv_buf"][chunk_id].at[step - 1],
            s["tm_send"].at[chunk_id, step - 1], s["tm_recv"].at[chunk_id, step - 1],
            device_id={"dp": me_dp, "tm": target}, device_id_type=MESH,
        )

    def when_owner(chunk_id, position, run):
        if owners(chunk_id) == p.tm:
            run()
        else:
            pl.when(position < owners(chunk_id))(run)

    def tm_send(chunk_id):
        stage_copy(chunk_id, p.bits - 1).wait_recv()
        add_block(chunk_id, p.bits, {b: bit_of[b] for b in range(p.bits)})
        for step in range(1, p.tm):
            when_owner(
                chunk_id, lax.rem(me_tm + step, p.tm), tm_copy(chunk_id, step).start
            )

    def finish(chunk_id):
        layer, parts, _, _ = p.chunks[chunk_id]
        at = g_index({b: bit_of[b] for b in range(p.bits)})

        def run():
            for step in range(1, p.tm):
                tm_copy(chunk_id, step).wait_recv()
            cols = pl.ds(pl.multiple_of(me_tm * p.width, LANES), p.width)
            total = s["grad"][chunk_id][at + (slice(None), cols)].astype(F32)
            for step in range(1, p.tm):
                total += s["tm_recv_buf"][chunk_id][step - 1].astype(F32)
            row = 0
            for part in parts:
                high = p.part_rows(part)
                piece = total[row : row + high]
                if part == "cond":
                    cond_o[layer] = piece
                elif part == "res":
                    res_o[layer] = piece
                else:
                    in_o[layer, part] = piece
                row += high

        when_owner(chunk_id, me_tm, run)

    def drain(chunk_id):
        for stage in range(p.bits):
            stage_copy(chunk_id, stage).wait_send()
        for step in range(1, p.tm):
            when_owner(
                chunk_id, lax.rem(me_tm + step, p.tm), tm_copy(chunk_id, step).wait_send
            )

    lane_iota = lax.broadcasted_iota(jnp.int32, (p.group, LANES), 1)
    row_iota = lax.broadcasted_iota(jnp.int32, (p.group, LANES), 0)
    loads["audio"].wait()
    halo_wait(0)
    halo_lanes = p.pad_rows - rows
    blocks = [jnp.zeros((p.group, LANES), F32) for _ in range(halo_lanes // LANES)]
    lane_ok = [jnp.zeros((p.group, LANES), jnp.int32) for _ in range(halo_lanes // LANES)]
    low_ok = jnp.where(has_low, 1, 0)
    high_ok = jnp.where(has_high, 1, 0)
    for clip in range(p.clips):
        at = clip * 2 * EDGE
        block, lane = at // LANES, at % LANES
        for slot in range(2):
            first = lane + slot * EDGE
            inside = (lane_iota >= first) & (lane_iota < first + EDGE)
            ok = low_ok if slot == 0 else high_ok
            turned = pltpu.roll(s["audio_halo"][slot, clip], (lane + EDGE) % LANES, 1)
            keep = inside & (jnp.broadcast_to(ok, inside.shape) > 0)
            blocks[block] = jnp.where(keep, turned, blocks[block])
            lane_ok[block] = jnp.where(keep, 1, lane_ok[block])
    audio_all = jnp.concatenate(
        [s["audio"][clip] for clip in range(p.clips)] + blocks, axis=1
    )
    main_ok = jnp.ones((p.group, rows), jnp.int32)
    inside_clip = jnp.concatenate([main_ok] + lane_ok, axis=1) > 0
    group_rows = lax.broadcasted_iota(jnp.int32, (p.group, p.pad_rows), 0)
    first8 = jnp.where(group_rows < p.half, audio_all, 0.0)
    s["first"][...] = first8[:, :rows]
    s["second"][...] = pltpu.roll(audio_all, p.half, 0)
    start8 = s["start8"]
    start8[...] = jnp.zeros_like(start8)
    start8[0 : p.half] = start_w[...]
    first_cols = jnp.transpose(first8, (1, 0))
    for block in range(ch // LANES):
        cols = slice(block * LANES, (block + 1) * LANES)
        s["state"][:, cols] = dot(
            first_cols[:all_rows], start8[:, cols], precision=HIGHEST
        )

    for clip in range(p.clips):
        loads[f"mel{clip}"].wait()
    halo_wait(1)
    for clip in range(p.clips):
        low = s["mel_halo"][0, clip].astype(F32)[EDGE:]
        high = s["mel_halo"][1, clip].astype(F32)[:EDGE]
        low = jnp.where(jnp.broadcast_to(low_ok, low.shape) > 0, low, 0.0)
        high = jnp.where(jnp.broadcast_to(high_ok, high.shape) > 0, high, 0.0)
        s["mel"][pl.ds(rows + clip * 2 * EDGE, 2 * EDGE)] = jnp.concatenate(
            [low, high], axis=0
        ).astype(BF16)

    def extended(ref, clip, cols):
        at = rows + clip * 2 * EDGE
        return jnp.concatenate(
            [
                ref[pl.ds(at, EDGE), cols],
                ref[pl.ds(clip * fr, fr), cols],
                ref[pl.ds(at + EDGE, EDGE), cols],
            ],
            axis=0,
        )

    def store_extended(ref, clip, cols, value):
        ref[pl.ds(clip * fr, fr), cols] = value[EDGE : EDGE + fr].astype(BF16)
        ref[pl.ds(rows + clip * 2 * EDGE, 2 * EDGE), cols] = jnp.concatenate(
            [value[:EDGE], value[EDGE + fr :]], axis=0
        ).astype(BF16)

    ext_iota = lax.broadcasted_iota(jnp.int32, (ext, LANES), 0)
    low_row = jnp.broadcast_to(me_tm == 0, (ext, LANES)) & (ext_iota < EDGE)
    high_row = jnp.broadcast_to(me_tm == p.tm - 1, (ext, LANES)) & (
        ext_iota >= EDGE + fr
    )
    outside = low_row | high_row

    def lanes_at(start):
        return pl.ds(pl.multiple_of(start, LANES), LANES)

    def block_at(start):
        return pl.ds(pl.multiple_of(start, BLOCK), BLOCK)

    def spread_state(layer):
        reach = 2**layer

        @pl.loop(0, ch // LANES)
        def _(block):
            for clip in range(p.clips):
                value = extended(s["state"], clip, lanes_at(block * LANES))
                value = jnp.where(outside, 0.0, value)
                for tap in range(p.taps):
                    shift = ((1 - tap) * reach) % ext
                    moved = pltpu.roll(value, shift, 0) if shift else value
                    store_extended(
                        s["taps"], clip, lanes_at(tap * ch + block * LANES), moved
                    )

        mid = p.taps // 2
        s["state_t"][layer] = jnp.transpose(
            s["taps"][0:rows, mid * ch : (mid + 1) * ch], (1, 0)
        )

    def gate(layer):
        @pl.loop(0, n_blocks)
        def _(n):
            pre = []
            for side in range(2):
                cols = block_at(side * ch + n * BLOCK)
                pre.append(
                    dot(s["taps"][...], s["win"][layer, :, cols])
                    + dot(s["mel"][...], s["cond"][layer, :, cols])
                )
            tangent = jnp.tanh(pre[0])
            switch = 0.5 * jnp.tanh(0.5 * pre[1]) + 0.5
            cols = block_at(n * BLOCK)
            s["tangent"][layer, :, cols] = tangent
            s["switch"][layer, :, cols] = switch
            s["gated"][layer, 0:all_rows, cols] = (tangent * switch).astype(BF16)

    def gate_back(layer):
        reach = 2**layer

        @pl.loop(0, ch // LANES)
        def _(block):
            cols = lanes_at(block * LANES)
            for clip in range(p.clips):
                up = extended(s["act"], clip, cols)
                tangent = extended(s["tangent"].at[layer], clip, cols)
                switch = extended(s["switch"].at[layer], clip, cols)
                lift = jnp.where(outside, 0.0, up) * switch
                sides = (
                    lift * (1.0 - tangent * tangent),
                    lift * tangent * (1.0 - switch),
                )
                for side in range(2):
                    for tap in range(p.taps):
                        shift = ((tap - 1) * reach) % ext
                        moved = pltpu.roll(sides[side], shift, 0) if shift else sides[side]
                        store_extended(
                            s["back"], clip,
                            lanes_at(tap * p.wide + side * ch + block * LANES), moved,
                        )

    def put_owned(chunk_id, row, high, cols, value):
        acc = s["grad"][chunk_id]
        for owner in range(p.dp):
            at = tuple((owner >> b) & 1 for b in reversed(range(p.bits)))
            acc[at + (pl.ds(row, high), cols)] = value[
                owner * high : (owner + 1) * high
            ].astype(BF16)

    def weight_grads(chunk_id):
        layer, parts, columns, _ = p.chunks[chunk_id]
        row = 0
        mid = p.taps // 2
        for part in parts:
            high = p.part_rows(part)

            def body(n, part=part, row=row, high=high):
                cols = block_at(n * BLOCK)
                if part == "cond":
                    left = s["mel_t"][...]
                    right = s["back"][0:rows, block_at(mid * p.wide + n * BLOCK)]
                elif part == "res":
                    left = jnp.transpose(s["gated"][layer, 0:rows, :], (1, 0))
                    right = s["join"][0:rows, cols]
                else:
                    left = s["state_t"][layer]
                    right = s["back"][0:rows, block_at(part * p.wide + n * BLOCK)]
                put_owned(chunk_id, row, high, cols, dot(left, right))

            pl.loop(0, columns // BLOCK)(body)
            row += high

    def state_grad(layer, accumulate):
        @pl.loop(0, n_blocks)
        def _(n):
            total = None
            for tap in range(p.taps):
                term = dot(
                    s["back"][:, tap * p.wide : (tap + 1) * p.wide],
                    s["win"][layer, block_at(tap * ch + n * BLOCK), :],
                    ((1,), (1,)),
                )
                total = term if total is None else total + term
            cols = block_at(n * BLOCK)
            if accumulate:
                total = total + s["state"][:, cols]
            s["state"][:, cols] = total

    spread_state(0)
    s["mel_t"][...] = jnp.transpose(s["mel"][0:rows, :], (1, 0))
    loads["win0"].wait()
    loads["cond0"].wait()
    gate(0)
    loads["res"].wait()

    @pl.loop(0, n_blocks)
    def _(n):
        cols = block_at(n * BLOCK)
        s["state"][:, cols] = s["state"][:, cols] + dot(
            s["gated"][0, 0:all_rows, :], s["res"][:, cols]
        )

    spread_state(1)
    loads["last"].wait()
    end_cols = jnp.transpose(end_w[...].astype(F32), (1, 0)).astype(BF16)
    skips = [
        dot(end_cols, s["res"][:, ch:], ((1,), (1,))),
        dot(end_cols, s["last"][...], ((1,), (1,))),
    ]
    for layer in range(p.layers):
        coarse = skips[layer].astype(BF16)
        fine = skips[layer] - coarse.astype(F32)
        s["skip_w"][layer] = jnp.concatenate(
            [coarse.astype(F32), fine], axis=0
        ).astype(BF16)
    loads["win1"].wait()
    loads["cond1"].wait()
    gate(1)

    out = None
    for layer in range(p.layers):
        term = dot(s["skip_w"][layer], s["gated"][layer], ((1,), (1,)))
        term = term[: p.group] + term[p.group :]
        out = term if out is None else out + term
    top = group_rows < p.half
    inside_top = top & inside_clip
    log_scale = jnp.where(inside_top, out, 0.0)
    shift_term = jnp.where(inside_top, pltpu.roll(out, p.half, 0), 0.0)
    growth = jnp.exp(log_scale)
    second = s["second"][...]
    latent = growth * second + shift_term
    scale_inv = 1.0 / (p.clips * p.dp)
    upper = (latent * growth * second - 1.0) * scale_inv
    lower = pltpu.roll(jnp.where(top, latent, 0.0), p.half, 0) * scale_inv
    grad_out = jnp.where(inside_clip, jnp.where(top, upper, lower), 0.0)
    s["scaled"][...] = (jnp.where(top, latent * growth, 0.0) * scale_inv)[:, :rows]
    for clip in range(p.clips):
        latent_o[clip] = latent[0 : p.half, clip * fr : (clip + 1) * fr]
    first = s["first"][...]
    head = (latent * latent)[:, :rows] * 0.5 - log_scale[:, :rows]
    loss = jnp.sum(
        jnp.where(top[:, :rows], head, 0.0) + 0.5 * first * first, keepdims=True
    )
    s["loss"][...] = jnp.broadcast_to(loss * scale_inv, s["loss"].shape)
    grad_twice = jnp.concatenate([grad_out, grad_out], axis=0).astype(BF16)
    grad_b = grad_out.astype(BF16)
    for layer in range(p.layers):
        s["small"][layer * p.group : (layer + 1) * p.group] = dot(
            grad_b[:, :rows], s["gated"][layer, 0:rows, :]
        )
    s["grad_cols"][...] = jnp.transpose(
        jnp.concatenate([grad_out, grad_out], axis=0), (1, 0)
    ).astype(BF16)

    s["act"][...] = dot(s["grad_cols"][0:all_rows], s["skip_w"][1])
    gate_back(1)
    weight_grads(0)
    dp_send(0, 0)
    weight_grads(1)
    dp_send(1, 0)
    dp_send(0, 1)
    state_grad(1, False)
    dp_send(1, 1)

    @pl.loop(0, ch // LANES)
    def _(block):
        cols = lanes_at(block * LANES)
        for clip in range(p.clips):
            value = jnp.where(outside, 0.0, extended(s["state"], clip, cols))
            store_extended(s["join"], clip, cols, value)

    weight_grads(2)
    dp_send(2, 0)

    @pl.loop(0, n_blocks)
    def _(n):
        cols = block_at(n * BLOCK)
        s["act"][:, cols] = dot(
            s["join"][...], s["res"][cols, 0:ch], ((1,), (1,))
        ) + dot(s["grad_cols"][0:all_rows], s["skip_w"][0, :, cols])

    gate_back(0)
    weight_grads(3)
    dp_send(3, 0)
    weight_grads(4)
    dp_send(4, 0)
    late_stages(p, dp_send, tm_send, finish)
    state_grad(0, True)

    small = s["small"]
    lead = 2 * p.group
    start_grad = dot(first, s["state"][0:rows], precision=HIGHEST)
    start_rows = lax.broadcasted_iota(jnp.int32, start_grad.shape, 0)
    small[lead : lead + p.group] = jnp.where(
        start_rows == p.half, jnp.broadcast_to(s["loss"][0:1, 0:1], start_grad.shape),
        start_grad,
    )

    def small_copy(stage):
        return pltpu.make_async_remote_copy(
            small, s["small_recv"].at[stage],
            s["small_send_sem"].at[stage], s["small_recv_sem"].at[stage],
            device_id=partner(stage), device_id_type=MESH,
        )

    def small_tm(step):
        return pltpu.make_async_remote_copy(
            small, s["small_tm"].at[me_tm],
            s["small_tm_send"].at[step - 1], s["small_tm_recv"].at[step - 1],
            device_id=peer(step), device_id_type=MESH,
        )

    def small_step(stage):
        small_copy(stage).wait()
        small[...] = small[...] + s["small_recv"][stage]

    small_copy(0).start()
    first_back = dot(start8[...], s["state"][0:rows], ((1,), (1,)), precision=HIGHEST)
    front = first_back + first * scale_inv
    back_rows = pltpu.roll(s["scaled"][...], p.half, 0)
    audio_grad = jnp.where(group_rows[:, :rows] < p.half, front, back_rows)
    for clip in range(p.clips):
        audio_o[clip] = audio_grad[:, clip * fr : (clip + 1) * fr]
    tail_stages(p, dp_send, tm_send, finish, small_copy, small_step, small_tm)

    s["small_tm"][me_tm] = small[...]
    for step in range(1, p.tm):
        small_tm(step).wait()
    total = s["small_tm"][0]
    for at in range(1, p.tm):
        total += s["small_tm"][at]
    m_first, m_last = total[: p.group], total[p.group : lead]
    loss_o[...] = total[lead + p.half : lead + p.half + 1, 0:1]
    start_o[...] = total[lead : lead + p.half]

    def split(value):
        coarse = value.astype(BF16)
        return coarse, (value - coarse.astype(F32)).astype(BF16)

    end_t = None
    for m, w in ((m_first, s["res"][:, ch:]), (m_last, s["last"][...])):
        for term in split(m):
            part = dot(term, w)
            end_t = part if end_t is None else end_t + part
    end_o[...] = jnp.transpose(end_t, (1, 0))
    end_rows = end_cols
    for m, out_ref in ((m_first, s["res_skip"]), (m_last, last_o)):
        coarse, fine = split(jnp.transpose(m, (1, 0)))
        out_ref[...] = dot(coarse, end_rows) + dot(fine, end_rows)
    res_owners = ch // p.width

    @pl.when(me_tm >= res_owners)
    def _():
        cols = pl.ds(
            pl.multiple_of((me_tm - res_owners) * p.width, LANES), p.width
        )
        at = pl.ds(pl.multiple_of(me_dp * p.own_ch, p.own_ch), p.own_ch)
        res_o[0] = s["res_skip"][at, cols]

    for chunk_id in range(len(p.chunks)):
        finish(chunk_id)

    for chunk_id in range(len(p.chunks)):
        drain(chunk_id)

    @pl.when(has_high)
    def _():
        for copy in to_high:
            copy.wait_send()

    @pl.when(has_low)
    def _():
        for copy in to_low:
            copy.wait_send()


def late_stages(p, dp_send, tm_send, finish):
    for stage in range(2, p.bits):
        dp_send(0, stage)
        dp_send(1, stage)
    for chunk in (2, 3, 4):
        dp_send(chunk, 1)


def tail_stages(p, dp_send, tm_send, finish, small_copy, small_step, small_tm):
    tm_send(0)
    tm_send(1)
    for stage in range(1, p.bits):
        small_step(stage - 1)
        small_copy(stage).start()
    small_step(p.bits - 1)
    for step in range(1, p.tm):
        small_tm(step).start()
    for stage in range(2, p.bits):
        for chunk in (2, 3, 4):
            dp_send(chunk, stage)
    for chunk in (2, 3, 4):
        tm_send(chunk)


def solution(mesh):
    def shards(
        audio, mel_frames, start_weight, input_weight, cond_weight, res_weight,
        last_weight, end_weight,
    ):
        p = Plan(mesh, audio, mel_frames, start_weight, input_weight)
        ch, wide, dp = p.channels, p.wide, p.dp
        vmem, anywhere = pltpu.VMEM, pl.BlockSpec(memory_space=pl.ANY)
        inside = pl.BlockSpec(memory_space=pltpu.VMEM)
        twos = (2,) * p.bits
        heights = [p.chunk_rows(chunk) for chunk in p.chunks]
        widths = [chunk[2] for chunk in p.chunks]
        n_chunks = len(p.chunks)
        sem = pltpu.SemaphoreType.DMA
        scratch = {
            "audio": vmem(audio.shape, F32),
            "audio_halo": vmem((2, p.clips, p.group, LANES), F32),
            "mel": vmem((p.all_rows, p.cond), BF16),
            "mel_halo": vmem((2, p.clips, 2 * EDGE, p.cond), BF16),
            "mel_t": vmem((p.cond, p.rows), BF16),
            "win": vmem((p.layers, p.taps * ch, wide), BF16),
            "cond": vmem((p.layers, p.cond, wide), BF16),
            "res": vmem((ch, wide), BF16),
            "last": vmem((ch, ch), BF16),
            "first": vmem((p.group, p.rows), F32),
            "second": vmem((p.group, p.pad_rows), F32),
            "scaled": vmem((p.group, p.rows), F32),
            "start8": vmem((p.group, ch), F32),
            "loss": vmem((p.group, LANES), F32),
            "state": vmem((p.all_rows, ch), F32),
            "act": vmem((p.all_rows, ch), F32),
            "taps": vmem((p.all_rows, p.taps * ch), BF16),
            "state_t": vmem((p.layers, ch, p.rows), BF16),
            "tangent": vmem((p.layers, p.all_rows, ch), F32),
            "switch": vmem((p.layers, p.all_rows, ch), F32),
            "gated": vmem((p.layers, p.pad_rows, ch), BF16),
            "skip_w": vmem((p.layers, 2 * p.group, ch), BF16),
            "grad_cols": vmem((p.pad_rows, 2 * p.group), BF16),
            "join": vmem((p.all_rows, ch), BF16),
            "back": vmem((p.all_rows, p.taps * wide), BF16),
            "res_skip": vmem((ch, ch), F32),
            "small": vmem((3 * p.group, ch), F32),
            "small_recv": vmem((p.bits, 3 * p.group, ch), F32),
            "small_tm": vmem((p.tm, 3 * p.group, ch), F32),
            "grad": [vmem(twos + (h, w), BF16) for h, w in zip(heights, widths)],
            "recv": [
                [vmem((2,) * (p.bits - 1 - st) + (h, w), BF16) for st in range(p.bits)]
                for h, w in zip(heights, widths)
            ],
            "tm_recv_buf": [vmem((p.tm - 1, h, p.width), BF16) for h in heights],
            "load_sem": sem((3 + p.clips + 2 * p.layers,)),
            "halo_send": sem((2, 2)),
            "halo_recv": sem((2, 2)),
            "dp_send": sem((n_chunks, p.bits)),
            "dp_recv": sem((n_chunks, p.bits)),
            "tm_send": sem((n_chunks, p.tm - 1)),
            "tm_recv": sem((n_chunks, p.tm - 1)),
            "small_send_sem": sem((p.bits,)),
            "small_recv_sem": sem((p.bits,)),
            "small_tm_send": sem((p.tm - 1,)),
            "small_tm_recv": sem((p.tm - 1,)),
        }
        leaves, tree = jax.tree.flatten(scratch)

        def entry(*refs):
            fixed = 8 + 9
            kernel(p, *refs[:fixed], jax.tree.unflatten(tree, refs[fixed:]))

        shape = jax.ShapeDtypeStruct
        outs = pl.pallas_call(
            entry,
            out_shape=[
                shape((p.clips, p.half, p.frames), F32),
                shape(audio.shape, F32),
                shape((1, 1), F32),
                shape((p.layers, p.taps, p.own_ch, p.width), F32),
                shape((p.layers, p.own_cond, p.width), F32),
                shape((p.layers - 1, p.own_ch, p.width), F32),
                shape(last_weight.shape, F32),
                shape(end_weight.shape, F32),
                shape(start_weight.shape, F32),
            ],
            in_specs=[
                anywhere, anywhere, inside, anywhere, anywhere, anywhere, anywhere, inside
            ],
            out_specs=[inside] * 9,
            scratch_shapes=leaves,
            compiler_params=pltpu.CompilerParams(
                collective_id=0, has_side_effects=True,
                vmem_limit_bytes=67_043_328,
            ),
            name="coupling_step",
        )(
            audio,
            mel_frames,
            start_weight,
            input_weight.reshape(p.layers, p.taps * ch, wide),
            cond_weight,
            res_weight.reshape(ch, wide),
            last_weight,
            end_weight,
        )
        outs = list(outs)
        outs[2] = outs[2].reshape(())
        return tuple(outs)

    return jax.shard_map(
        shards,
        mesh=mesh,
        in_specs=(P("dp", None, "tm"), P("dp", "tm", None), P(), P(), P(), P(), P(), P()),
        out_specs=(
            P("dp", None, "tm"),
            P("dp", None, "tm"),
            P(),
            P(None, None, "dp", "tm"),
            P(None, "dp", "tm"),
            P(None, "dp", "tm"),
            P(),
            P(),
            P(),
        ),
        check_vma=False,
    )
```

```python
import itertools
import types

import jax
import jax.numpy as jnp
from jax import lax
from jax.experimental import pallas as pl
from jax.experimental.pallas import tpu as pltpu
from jax.sharding import PartitionSpec as P

F32 = jnp.float32
BF16 = jnp.bfloat16
HIGHEST = lax.Precision.HIGHEST
MESH = pl.DeviceIdType.MESH


EDGE = 8
BLOCK = 256
LANES = 128


def dot(a, b, dims=((1,), (0,)), precision=None):
    return lax.dot_general(
        a, b, (dims, ((), ())), precision=precision, preferred_element_type=F32
    )


def round_up(value, unit):
    return -(-value // unit) * unit


class Plan:
    def __init__(self, mesh, audio, mel, start_weight, input_weight):
        self.dp, self.tm = mesh.shape["dp"], mesh.shape["tm"]
        self.bits = self.dp.bit_length() - 1
        self.clips, self.group, self.frames = audio.shape
        self.half = self.group // 2
        self.cond = mel.shape[2]
        self.channels = start_weight.shape[1]
        self.layers, self.taps = input_weight.shape[:2]
        self.wide = 2 * self.channels
        self.rows = self.clips * self.frames
        self.all_rows = self.rows + self.clips * 2 * EDGE
        self.pad_rows = round_up(self.all_rows, LANES)
        self.own_ch = self.channels // self.dp
        self.own_cond = self.cond // self.dp
        self.width = self.wide // self.tm
        order = list(range(self.bits))
        self.first = order
        self.second = order[:1] + order[1:][::-1]
        tap_pair = tuple(range(self.taps - 1))
        rest = (self.taps - 1, "cond")
        self.chunks = [
            (1, tap_pair, self.wide, self.first),
            (1, rest, self.wide, self.second),
            (0, ("res",), self.channels, self.second),
            (0, tap_pair, self.wide, self.first),
            (0, rest, self.wide, self.second),
        ]

    def part_rows(self, part):
        return self.own_cond if part == "cond" else self.own_ch

    def chunk_rows(self, chunk):
        return round_up(sum(self.part_rows(part) for part in chunk[1]), 16)


def kernel(plan, *refs):
    p = plan
    n_in, n_out = 8, 7
    (audio_h, mel_h, start_w, win_h, cond_h, res_h, last_h, end_w) = refs[:n_in]
    latent_o, audio_o, in_o, cond_o, res_o, small_o, end_o = refs[n_in : n_in + n_out]
    s = refs[n_in + n_out]
    me_dp, me_tm = lax.axis_index("dp"), lax.axis_index("tm")
    bit_of = [(me_dp // 2**b) % 2 for b in range(p.bits)]
    ch, rows, all_rows, fr = p.channels, p.rows, p.all_rows, p.frames
    ext = fr + 2 * EDGE
    n_blocks = ch // BLOCK

    def partner(b):
        return {"dp": me_dp + (2**b) * (1 - 2 * bit_of[b]), "tm": me_tm}

    def peer(step):
        return {"dp": me_dp, "tm": lax.rem(me_tm + step, p.tm)}

    def load(src, dst, index):
        copy = pltpu.make_async_copy(src, dst, s.load_sem.at[index])
        copy.start()
        return copy

    audio_load = load(audio_h, s.audio, 0)
    mel_loads = [
        load(mel_h.at[clip], s.mel.at[pl.ds(clip * fr, fr)], 1 + clip)
        for clip in range(p.clips)
    ]
    base = 1 + p.clips
    weight_loads = []
    for layer in range(p.layers):
        at = base + 2 * layer
        weight_loads.append(
            [
                load(win_h.at[layer], s.win.at[layer], at),
                load(cond_h.at[layer], s.cond.at[layer], at + 1),
            ]
        )
        if layer == 0:
            res_load = load(res_h, s.res, base + 2 * p.layers)
            last_load = load(last_h, s.last, base + 2 * p.layers + 1)

    barrier = pltpu.get_barrier_semaphore()
    for b in range(p.bits):
        pl.semaphore_signal(barrier, 1, device_id=partner(b), device_id_type=MESH)
    for step in range(1, p.tm):
        pl.semaphore_signal(barrier, 1, device_id=peer(step), device_id_type=MESH)
    pl.semaphore_wait(barrier, p.bits + p.tm - 1)

    has_low, has_high = me_tm > 0, me_tm < p.tm - 1

    def halo_copies(slot):
        device = {"dp": me_dp, "tm": me_tm + 1 if slot == 0 else me_tm - 1}
        mel_at = fr - 2 * EDGE if slot == 0 else 0
        audio_at = fr - LANES if slot == 0 else 0
        return [
            pltpu.make_async_remote_copy(
                audio_h.at[:, :, pl.ds(audio_at, LANES)],
                s.audio_halo.at[slot],
                s.halo_send.at[slot, 0], s.halo_recv.at[slot, 0],
                device_id=device, device_id_type=MESH,
            ),
            pltpu.make_async_remote_copy(
                mel_h.at[:, pl.ds(mel_at, 2 * EDGE)],
                s.mel_halo.at[slot],
                s.halo_send.at[slot, 1], s.halo_recv.at[slot, 1],
                device_id=device, device_id_type=MESH,
            ),
        ]

    to_high, to_low = halo_copies(0), halo_copies(1)

    @pl.when(has_high)
    def _():
        for copy in to_high:
            copy.start()

    @pl.when(has_low)
    def _():
        for copy in to_low:
            copy.start()

    def halo_wait(index):
        @pl.when(has_low)
        def _():
            to_high[index].wait_recv()

        @pl.when(has_high)
        def _():
            to_low[index].wait_recv()

    def free_bits(order, stage):
        done = set(order[:stage])
        return [b for b in reversed(range(p.bits)) if b not in done]

    def g_index(values):
        return tuple(values[b] for b in reversed(range(p.bits)))

    def g_blocks(chunk_id, stage, other):
        order = p.chunks[chunk_id][3]
        bit = order[stage]
        free = free_bits(order, stage + 1)
        for combo in itertools.product((0, 1), repeat=len(free)):
            values = {b: bit_of[b] for b in order[:stage]}
            values[bit] = 1 - bit_of[bit] if other else bit_of[bit]
            values.update(zip(free, combo))
            yield values

    def recv_index(order, stage, values):
        return tuple(values[b] for b in free_bits(order, stage + 1))

    def add_block(chunk_id, stages, values):
        order = p.chunks[chunk_id][3]
        acc = s.grad[chunk_id]
        at = g_index(values)
        height = acc.shape[-2]

        @pl.loop(0, height // 16)
        def _(r):
            where = (pl.ds(pl.multiple_of(r * 16, 16), 16),)
            total = acc[at + where].astype(F32)
            for stage in range(stages):
                buf = s.recv[chunk_id][stage]
                total += buf[recv_index(order, stage, values) + where].astype(F32)
            acc[at + where] = total.astype(BF16)

    def stage_copy(chunk_id, stage):
        order = p.chunks[chunk_id][3]
        bit = order[stage]
        values = {b: slice(None) for b in range(p.bits)}
        values.update({b: bit_of[b] for b in order[:stage]})
        values[bit] = 1 - bit_of[bit]
        return pltpu.make_async_remote_copy(
            s.grad[chunk_id].at[g_index(values)],
            s.recv[chunk_id][stage],
            s.dp_send.at[chunk_id, stage], s.dp_recv.at[chunk_id, stage],
            device_id=partner(bit), device_id_type=MESH,
        )

    def dp_send(chunk_id, stage):
        if stage:
            stage_copy(chunk_id, stage - 1).wait_recv()
            for values in g_blocks(chunk_id, stage, True):
                add_block(chunk_id, stage, values)
        stage_copy(chunk_id, stage).start()

    def owners(chunk_id):
        return p.chunks[chunk_id][2] // p.width

    def tm_copy(chunk_id, step):
        target = lax.rem(me_tm + step, p.tm)
        at = g_index({b: bit_of[b] for b in range(p.bits)})
        place = lax.rem(target, owners(chunk_id))
        cols = pl.ds(pl.multiple_of(place * p.width, LANES), p.width)
        return pltpu.make_async_remote_copy(
            s.grad[chunk_id].at[at + (slice(None), cols)],
            s.tm_recv_buf[chunk_id].at[step - 1],
            s.tm_send.at[chunk_id, step - 1], s.tm_recv.at[chunk_id, step - 1],
            device_id={"dp": me_dp, "tm": target}, device_id_type=MESH,
        )

    def when_owner(chunk_id, position, run):
        if owners(chunk_id) == p.tm:
            run()
        else:
            pl.when(position < owners(chunk_id))(run)

    def tm_send(chunk_id):
        stage_copy(chunk_id, p.bits - 1).wait_recv()
        add_block(chunk_id, p.bits, {b: bit_of[b] for b in range(p.bits)})
        for step in range(1, p.tm):
            when_owner(
                chunk_id, lax.rem(me_tm + step, p.tm), tm_copy(chunk_id, step).start
            )

    def finish(chunk_id):
        layer, parts, _, _ = p.chunks[chunk_id]
        at = g_index({b: bit_of[b] for b in range(p.bits)})

        def run():
            for step in range(1, p.tm):
                tm_copy(chunk_id, step).wait_recv()
            cols = pl.ds(pl.multiple_of(me_tm * p.width, LANES), p.width)
            total = s.grad[chunk_id][at + (slice(None), cols)].astype(F32)
            for step in range(1, p.tm):
                total += s.tm_recv_buf[chunk_id][step - 1].astype(F32)
            row = 0
            for part in parts:
                high = p.part_rows(part)
                piece = total[row : row + high]
                if part == "cond":
                    cond_o[layer] = piece
                elif part == "res":
                    res_o[layer] = piece
                else:
                    in_o[layer, part] = piece
                row += high

        when_owner(chunk_id, me_tm, run)

    def drain(chunk_id):
        for stage in range(p.bits):
            stage_copy(chunk_id, stage).wait_send()
        for step in range(1, p.tm):
            when_owner(
                chunk_id, lax.rem(me_tm + step, p.tm), tm_copy(chunk_id, step).wait_send
            )

    lane_iota = lax.broadcasted_iota(jnp.int32, (p.group, LANES), 1)
    row_iota = lax.broadcasted_iota(jnp.int32, (p.group, LANES), 0)
    audio_load.wait()
    halo_wait(0)
    halo_lanes = p.pad_rows - rows
    blocks = [jnp.zeros((p.group, LANES), F32) for _ in range(halo_lanes // LANES)]
    lane_ok = [jnp.zeros((p.group, LANES), jnp.int32) for _ in range(halo_lanes // LANES)]
    low_ok = jnp.where(has_low, 1, 0)
    high_ok = jnp.where(has_high, 1, 0)
    for clip in range(p.clips):
        at = clip * 2 * EDGE
        block, lane = at // LANES, at % LANES
        for slot in range(2):
            first = lane + slot * EDGE
            inside = (lane_iota >= first) & (lane_iota < first + EDGE)
            ok = low_ok if slot == 0 else high_ok
            turned = pltpu.roll(s.audio_halo[slot, clip], (lane + EDGE) % LANES, 1)
            keep = inside & (jnp.broadcast_to(ok, inside.shape) > 0)
            blocks[block] = jnp.where(keep, turned, blocks[block])
            lane_ok[block] = jnp.where(keep, 1, lane_ok[block])
    audio_all = jnp.concatenate(
        [s.audio[clip] for clip in range(p.clips)] + blocks, axis=1
    )
    main_ok = jnp.ones((p.group, rows), jnp.int32)
    inside_clip = jnp.concatenate([main_ok] + lane_ok, axis=1) > 0
    group_rows = lax.broadcasted_iota(jnp.int32, (p.group, p.pad_rows), 0)
    first8 = jnp.where(group_rows < p.half, audio_all, 0.0)
    s.first[...] = first8[:, :rows]
    s.second[...] = pltpu.roll(audio_all, p.half, 0)
    start8 = s.start8
    start8[...] = jnp.zeros_like(start8)
    start8[0 : p.half] = start_w[...]
    first_cols = jnp.transpose(first8, (1, 0))
    for block in range(ch // LANES):
        cols = slice(block * LANES, (block + 1) * LANES)
        s.state[:, cols] = dot(
            first_cols[:all_rows], start8[:, cols], precision=HIGHEST
        )

    for clip in range(p.clips):
        mel_loads[clip].wait()
    halo_wait(1)
    for clip in range(p.clips):
        low = s.mel_halo[0, clip].astype(F32)[EDGE:]
        high = s.mel_halo[1, clip].astype(F32)[:EDGE]
        low = jnp.where(jnp.broadcast_to(low_ok, low.shape) > 0, low, 0.0)
        high = jnp.where(jnp.broadcast_to(high_ok, high.shape) > 0, high, 0.0)
        s.mel[pl.ds(rows + clip * 2 * EDGE, 2 * EDGE)] = jnp.concatenate(
            [low, high], axis=0
        ).astype(BF16)

    def extended(ref, clip, cols):
        at = rows + clip * 2 * EDGE
        return jnp.concatenate(
            [
                ref[pl.ds(at, EDGE), cols],
                ref[pl.ds(clip * fr, fr), cols],
                ref[pl.ds(at + EDGE, EDGE), cols],
            ],
            axis=0,
        )

    def store_extended(ref, clip, cols, value):
        ref[pl.ds(clip * fr, fr), cols] = value[EDGE : EDGE + fr].astype(BF16)
        ref[pl.ds(rows + clip * 2 * EDGE, 2 * EDGE), cols] = jnp.concatenate(
            [value[:EDGE], value[EDGE + fr :]], axis=0
        ).astype(BF16)

    ext_iota = lax.broadcasted_iota(jnp.int32, (ext, LANES), 0)
    low_row = jnp.broadcast_to(me_tm == 0, (ext, LANES)) & (ext_iota < EDGE)
    high_row = jnp.broadcast_to(me_tm == p.tm - 1, (ext, LANES)) & (
        ext_iota >= EDGE + fr
    )
    outside = low_row | high_row

    def lanes_at(start):
        return pl.ds(pl.multiple_of(start, LANES), LANES)

    def block_at(start):
        return pl.ds(pl.multiple_of(start, BLOCK), BLOCK)

    def spread_state(layer):
        reach = 2**layer

        @pl.loop(0, ch // LANES)
        def _(block):
            for clip in range(p.clips):
                value = extended(s.state, clip, lanes_at(block * LANES))
                value = jnp.where(outside, 0.0, value)
                for tap in range(p.taps):
                    shift = ((1 - tap) * reach) % ext
                    moved = pltpu.roll(value, shift, 0) if shift else value
                    store_extended(
                        s.taps, clip, lanes_at(tap * ch + block * LANES), moved
                    )

        mid = p.taps // 2
        s.state_t[layer] = jnp.transpose(
            s.taps[0:rows, mid * ch : (mid + 1) * ch], (1, 0)
        )

    def gate(layer):
        @pl.loop(0, n_blocks)
        def _(n):
            pre = []
            for side in range(2):
                cols = block_at(side * ch + n * BLOCK)
                pre.append(
                    dot(s.taps[...], s.win[layer, :, cols])
                    + dot(s.mel[...], s.cond[layer, :, cols])
                )
            tangent = jnp.tanh(pre[0])
            switch = 0.5 * jnp.tanh(0.5 * pre[1]) + 0.5
            cols = block_at(n * BLOCK)
            s.tangent[layer, :, cols] = tangent
            s.switch[layer, :, cols] = switch
            s.gated[layer, 0:all_rows, cols] = (tangent * switch).astype(BF16)

    def gate_back(layer):
        reach = 2**layer

        @pl.loop(0, ch // LANES)
        def _(block):
            cols = lanes_at(block * LANES)
            for clip in range(p.clips):
                up = extended(s.act, clip, cols)
                tangent = extended(s.tangent.at[layer], clip, cols)
                switch = extended(s.switch.at[layer], clip, cols)
                lift = jnp.where(outside, 0.0, up) * switch
                sides = (
                    lift * (1.0 - tangent * tangent),
                    lift * tangent * (1.0 - switch),
                )
                for side in range(2):
                    for tap in range(p.taps):
                        shift = ((tap - 1) * reach) % ext
                        moved = pltpu.roll(sides[side], shift, 0) if shift else sides[side]
                        store_extended(
                            s.back, clip,
                            lanes_at(tap * p.wide + side * ch + block * LANES), moved,
                        )

    def put_owned(chunk_id, row, high, cols, value):
        acc = s.grad[chunk_id]
        for owner in range(p.dp):
            at = tuple((owner >> b) & 1 for b in reversed(range(p.bits)))
            acc[at + (pl.ds(row, high), cols)] = value[
                owner * high : (owner + 1) * high
            ].astype(BF16)

    def weight_grads(chunk_id):
        layer, parts, columns, _ = p.chunks[chunk_id]
        row = 0
        mid = p.taps // 2
        for part in parts:
            high = p.part_rows(part)

            def body(n, part=part, row=row, high=high):
                cols = block_at(n * BLOCK)
                if part == "cond":
                    left = s.mel_t[...]
                    right = s.back[0:rows, block_at(mid * p.wide + n * BLOCK)]
                elif part == "res":
                    left = jnp.transpose(s.gated[layer, 0:rows, :], (1, 0))
                    right = s.join[0:rows, cols]
                else:
                    left = s.state_t[layer]
                    right = s.back[0:rows, block_at(part * p.wide + n * BLOCK)]
                put_owned(chunk_id, row, high, cols, dot(left, right))

            pl.loop(0, columns // BLOCK)(body)
            row += high

    def state_grad(layer, accumulate):
        @pl.loop(0, n_blocks)
        def _(n):
            total = None
            for tap in range(p.taps):
                term = dot(
                    s.back[:, tap * p.wide : (tap + 1) * p.wide],
                    s.win[layer, block_at(tap * ch + n * BLOCK), :],
                    ((1,), (1,)),
                )
                total = term if total is None else total + term
            cols = block_at(n * BLOCK)
            if accumulate:
                total = total + s.state[:, cols]
            s.state[:, cols] = total

    spread_state(0)
    s.mel_t[...] = jnp.transpose(s.mel[0:rows, :], (1, 0))
    for copy in weight_loads[0]:
        copy.wait()
    gate(0)
    res_load.wait()

    @pl.loop(0, n_blocks)
    def _(n):
        cols = block_at(n * BLOCK)
        s.state[:, cols] = s.state[:, cols] + dot(
            s.gated[0, 0:all_rows, :], s.res[:, cols]
        )

    spread_state(1)
    last_load.wait()
    end_cols = end_w[...]
    skips = [
        dot(end_cols, s.res[:, ch:], ((1,), (1,))),
        dot(end_cols, s.last[...], ((1,), (1,))),
    ]
    for layer in range(p.layers):
        coarse = skips[layer].astype(BF16)
        fine = skips[layer] - coarse.astype(F32)
        s.skip_w[layer] = jnp.concatenate(
            [coarse.astype(F32), fine], axis=0
        ).astype(BF16)
    for copy in weight_loads[1]:
        copy.wait()
    gate(1)

    out = None
    for layer in range(p.layers):
        term = dot(s.skip_w[layer], s.gated[layer], ((1,), (1,)))
        term = term[: p.group] + term[p.group :]
        out = term if out is None else out + term
    top = group_rows < p.half
    inside_top = top & inside_clip
    log_scale = jnp.where(inside_top, out, 0.0)
    shift_term = jnp.where(inside_top, pltpu.roll(out, p.half, 0), 0.0)
    growth = jnp.exp(log_scale)
    second = s.second[...]
    latent = growth * second + shift_term
    scale_inv = 1.0 / (p.clips * p.dp)
    upper = (latent * growth * second - 1.0) * scale_inv
    lower = pltpu.roll(jnp.where(top, latent, 0.0), p.half, 0) * scale_inv
    grad_out = jnp.where(inside_clip, jnp.where(top, upper, lower), 0.0)
    s.scaled[...] = (jnp.where(top, latent * growth, 0.0) * scale_inv)[:, :rows]
    for clip in range(p.clips):
        latent_o[clip] = latent[0 : p.half, clip * fr : (clip + 1) * fr]
    first = s.first[...]
    head = (latent * latent)[:, :rows] * 0.5 - log_scale[:, :rows]
    loss = jnp.sum(
        jnp.where(top[:, :rows], head, 0.0) + 0.5 * first * first, keepdims=True
    )
    s.loss[...] = jnp.broadcast_to(loss * scale_inv, s.loss.shape)
    grad_twice = jnp.concatenate([grad_out, grad_out], axis=0).astype(BF16)
    grad_b = grad_out.astype(BF16)
    for layer in range(p.layers):
        s.small[layer * p.group : (layer + 1) * p.group] = dot(
            grad_b[:, :rows], s.gated[layer, 0:rows, :]
        )
    s.grad_cols[...] = jnp.transpose(
        jnp.concatenate([grad_out, grad_out], axis=0), (1, 0)
    ).astype(BF16)

    s.act[...] = dot(s.grad_cols[0:all_rows], s.skip_w[1])
    gate_back(1)
    weight_grads(0)
    dp_send(0, 0)
    weight_grads(1)
    dp_send(1, 0)
    dp_send(0, 1)
    state_grad(1, False)
    dp_send(1, 1)

    @pl.loop(0, ch // LANES)
    def _(block):
        cols = lanes_at(block * LANES)
        for clip in range(p.clips):
            value = jnp.where(outside, 0.0, extended(s.state, clip, cols))
            store_extended(s.join, clip, cols, value)

    weight_grads(2)
    dp_send(2, 0)

    @pl.loop(0, n_blocks)
    def _(n):
        cols = block_at(n * BLOCK)
        s.act[:, cols] = dot(
            s.join[...], s.res[cols, 0:ch], ((1,), (1,))
        ) + dot(s.grad_cols[0:all_rows], s.skip_w[0, :, cols])

    gate_back(0)
    weight_grads(3)
    dp_send(3, 0)
    weight_grads(4)
    dp_send(4, 0)
    late_stages(p, dp_send, tm_send, finish)
    state_grad(0, True)

    small = s.small
    lead = 2 * p.group
    start_grad = dot(first, s.state[0:rows], precision=HIGHEST)
    start_rows = lax.broadcasted_iota(jnp.int32, start_grad.shape, 0)
    small[lead : lead + p.group] = jnp.where(
        start_rows == p.half, jnp.broadcast_to(s.loss[0:1, 0:1], start_grad.shape),
        start_grad,
    )

    def small_copy(stage):
        return pltpu.make_async_remote_copy(
            small, s.small_recv.at[stage],
            s.small_send_sem.at[stage], s.small_recv_sem.at[stage],
            device_id=partner(stage), device_id_type=MESH,
        )

    def small_tm(step):
        return pltpu.make_async_remote_copy(
            small, s.small_tm.at[me_tm],
            s.small_tm_send.at[step - 1], s.small_tm_recv.at[step - 1],
            device_id=peer(step), device_id_type=MESH,
        )

    def small_step(stage):
        small_copy(stage).wait()
        small[...] = small[...] + s.small_recv[stage]

    small_copy(0).start()
    first_back = dot(start8[...], s.state[0:rows], ((1,), (1,)), precision=HIGHEST)
    front = first_back + first * scale_inv
    back_rows = pltpu.roll(s.scaled[...], p.half, 0)
    audio_grad = jnp.where(group_rows[:, :rows] < p.half, front, back_rows)
    for clip in range(p.clips):
        audio_o[clip] = audio_grad[:, clip * fr : (clip + 1) * fr]
    tail_stages(p, dp_send, tm_send, finish, small_copy, small_step, small_tm)

    s.small_tm[me_tm] = small[...]
    for step in range(1, p.tm):
        small_tm(step).wait()
    total = s.small_tm[0]
    for at in range(1, p.tm):
        total += s.small_tm[at]
    m_first, m_last = total[: p.group], total[p.group : lead]
    small_o[...] = total
    end_t = None
    for m, w in ((m_first, s.res[:, ch:]), (m_last, s.last[...])):
        for term in split(m):
            part = dot(term, w)
            end_t = part if end_t is None else end_t + part
    end_o[...] = end_t

    for chunk_id in range(len(p.chunks)):
        finish(chunk_id)

    for chunk_id in range(len(p.chunks)):
        drain(chunk_id)

    @pl.when(has_high)
    def _():
        for copy in to_high:
            copy.wait_send()

    @pl.when(has_low)
    def _():
        for copy in to_low:
            copy.wait_send()


def split(value):
    coarse = value.astype(BF16)
    return coarse, (value - coarse.astype(F32)).astype(BF16)


def outputs_kernel(plan, *refs):
    p = plan
    (latent_i, audio_i, in_i, cond_i, res_i, small_i, end_i, end_w) = refs[:8]
    (
        latent_o, audio_o, loss_o, in_o, cond_o, res_o, last_o, end_o, start_o, skip
    ) = refs[8:]
    me_dp, me_tm = lax.axis_index("dp"), lax.axis_index("tm")
    lead = 2 * p.group
    for source, target in (
        (latent_i, latent_o), (audio_i, audio_o), (in_i, in_o), (cond_i, cond_o),
        (end_i, end_o),
    ):
        target[...] = source[...]
    loss_o[...] = small_i[lead + p.half : lead + p.half + 1, 0:1]
    start_o[...] = small_i[lead : lead + p.half]
    end_rows = end_w[...]
    for at, out_ref in ((0, skip), (p.group, last_o)):
        m_cols = jnp.transpose(small_i[at : at + p.group], (1, 0))
        coarse, fine = split(m_cols)
        out_ref[...] = dot(coarse, end_rows) + dot(fine, end_rows)
    res_owners = p.channels // p.width

    @pl.when(me_tm < res_owners)
    def _():
        res_o[...] = res_i[...]

    @pl.when(me_tm >= res_owners)
    def _():
        cols = pl.ds(pl.multiple_of((me_tm - res_owners) * p.width, LANES), p.width)
        at = pl.ds(pl.multiple_of(me_dp * p.own_ch, p.own_ch), p.own_ch)
        res_o[0] = skip[at, cols]


def late_stages(p, dp_send, tm_send, finish):
    for stage in range(2, p.bits):
        dp_send(0, stage)
        dp_send(1, stage)
    for chunk in (2, 3, 4):
        dp_send(chunk, 1)


def tail_stages(p, dp_send, tm_send, finish, small_copy, small_step, small_tm):
    tm_send(0)
    tm_send(1)
    for stage in range(1, p.bits):
        small_step(stage - 1)
        small_copy(stage).start()
    small_step(p.bits - 1)
    for step in range(1, p.tm):
        small_tm(step).start()
    for stage in range(2, p.bits):
        for chunk in (2, 3, 4):
            dp_send(chunk, stage)
    for chunk in (2, 3, 4):
        tm_send(chunk)


def solution(mesh):
    def shards(
        audio, mel_frames, start_weight, input_weight, cond_weight, res_weight,
        last_weight, end_weight,
    ):
        p = Plan(mesh, audio, mel_frames, start_weight, input_weight)
        ch, wide, dp = p.channels, p.wide, p.dp
        vmem, anywhere = pltpu.VMEM, pl.BlockSpec(memory_space=pl.ANY)
        inside = pl.BlockSpec(memory_space=pltpu.VMEM)
        twos = (2,) * p.bits
        heights = [p.chunk_rows(chunk) for chunk in p.chunks]
        widths = [chunk[2] for chunk in p.chunks]
        n_chunks = len(p.chunks)
        sem = pltpu.SemaphoreType.DMA
        scratch = dict(
            audio=vmem(audio.shape, F32),
            audio_halo=vmem((2, p.clips, p.group, LANES), F32),
            mel=vmem((p.all_rows, p.cond), BF16),
            mel_halo=vmem((2, p.clips, 2 * EDGE, p.cond), BF16),
            mel_t=vmem((p.cond, p.rows), BF16),
            win=vmem((p.layers, p.taps * ch, wide), BF16),
            cond=vmem((p.layers, p.cond, wide), BF16),
            res=vmem((ch, wide), BF16),
            last=vmem((ch, ch), BF16),
            first=vmem((p.group, p.rows), F32),
            second=vmem((p.group, p.pad_rows), F32),
            scaled=vmem((p.group, p.rows), F32),
            start8=vmem((p.group, ch), F32),
            loss=vmem((p.group, LANES), F32),
            state=vmem((p.all_rows, ch), F32),
            act=vmem((p.all_rows, ch), F32),
            taps=vmem((p.all_rows, p.taps * ch), BF16),
            state_t=vmem((p.layers, ch, p.rows), BF16),
            tangent=vmem((p.layers, p.all_rows, ch), F32),
            switch=vmem((p.layers, p.all_rows, ch), F32),
            gated=vmem((p.layers, p.pad_rows, ch), BF16),
            skip_w=vmem((p.layers, 2 * p.group, ch), BF16),
            grad_cols=vmem((p.pad_rows, 2 * p.group), BF16),
            join=vmem((p.all_rows, ch), BF16),
            back=vmem((p.all_rows, p.taps * wide), BF16),
            small=vmem((3 * p.group, ch), F32),
            small_recv=vmem((p.bits, 3 * p.group, ch), F32),
            small_tm=vmem((p.tm, 3 * p.group, ch), F32),
            grad=[vmem(twos + (h, w), BF16) for h, w in zip(heights, widths)],
            recv=[
                [vmem((2,) * (p.bits - 1 - st) + (h, w), BF16) for st in range(p.bits)]
                for h, w in zip(heights, widths)
            ],
            tm_recv_buf=[vmem((p.tm - 1, h, p.width), BF16) for h in heights],
            load_sem=sem((3 + p.clips + 2 * p.layers,)),
            halo_send=sem((2, 2)),
            halo_recv=sem((2, 2)),
            dp_send=sem((n_chunks, p.bits)),
            dp_recv=sem((n_chunks, p.bits)),
            tm_send=sem((n_chunks, p.tm - 1)),
            tm_recv=sem((n_chunks, p.tm - 1)),
            small_send_sem=sem((p.bits,)),
            small_recv_sem=sem((p.bits,)),
            small_tm_send=sem((p.tm - 1,)),
            small_tm_recv=sem((p.tm - 1,)),
        )
        leaves, tree = jax.tree.flatten(scratch)

        def entry(*refs):
            fixed = 8 + 7
            names = types.SimpleNamespace(**jax.tree.unflatten(tree, refs[fixed:]))
            kernel(p, *refs[:fixed], names)

        shape = jax.ShapeDtypeStruct
        latent = shape((p.clips, p.half, p.frames), F32)
        audio_grad = shape(audio.shape, F32)
        in_grad = shape((p.layers, p.taps, p.own_ch, p.width), F32)
        cond_grad = shape((p.layers, p.own_cond, p.width), F32)
        res_grad = shape((p.layers - 1, p.own_ch, p.width), F32)
        end_grad = shape((p.group, ch), F32)
        end_t = end_weight.T
        held = pl.pallas_call(
            entry,
            out_shape=[
                latent, audio_grad, in_grad, cond_grad, res_grad,
                shape((3 * p.group, ch), F32), end_grad,
            ],
            in_specs=[
                anywhere, anywhere, inside, anywhere, anywhere, anywhere, anywhere, inside
            ],
            out_specs=[inside] * 7,
            scratch_shapes=leaves,
            compiler_params=pltpu.CompilerParams(
                collective_id=0, has_side_effects=True,
                vmem_limit_bytes=67_043_328,
            ),
            name="coupling_step",
        )(
            audio,
            mel_frames,
            start_weight,
            input_weight.reshape(p.layers, p.taps * ch, wide),
            cond_weight,
            res_weight.reshape(ch, wide),
            last_weight,
            end_t,
        )
        outs = pl.pallas_call(
            lambda *refs: outputs_kernel(p, *refs),
            out_shape=[
                latent, audio_grad, shape((1, 1), F32), in_grad, cond_grad, res_grad,
                shape(last_weight.shape, F32), end_grad, shape(start_weight.shape, F32),
            ],
            in_specs=[inside] * 8,
            out_specs=[inside] * 9,
            scratch_shapes=[vmem((ch, ch), F32)],
            name="coupling_outputs",
        )(*held, end_t)
        outs = list(outs)
        outs[2] = outs[2].reshape(())
        outs[7] = outs[7].T
        return tuple(outs)

    return jax.shard_map(
        shards,
        mesh=mesh,
        in_specs=(P("dp", None, "tm"), P("dp", "tm", None), P(), P(), P(), P(), P(), P()),
        out_specs=(
            P("dp", None, "tm"),
            P("dp", None, "tm"),
            P(),
            P(None, None, "dp", "tm"),
            P(None, "dp", "tm"),
            P(None, "dp", "tm"),
            P(),
            P(),
            P(),
        ),
        check_vma=False,
    )
```

```python
import itertools
import types

import jax
import jax.numpy as jnp
from jax import lax
from jax.experimental import pallas as pl
from jax.experimental.pallas import tpu as pltpu
from jax.sharding import PartitionSpec as P

F32 = jnp.float32
BF16 = jnp.bfloat16
HIGHEST = lax.Precision.HIGHEST
MESH = pl.DeviceIdType.MESH


EDGE = 8
BLOCK = 256
GRAD_BLOCK = 512
LANES = 128
COND, RES = -1, -2


def dot(a, b, dims=((1,), (0,)), precision=None):
    return lax.dot_general(
        a, b, (dims, ((), ())), precision=precision, preferred_element_type=F32
    )


def round_up(value, unit):
    return -(-value // unit) * unit


class Plan:
    def __init__(self, mesh, audio, mel, start_weight, input_weight):
        self.dp, self.tm = mesh.shape["dp"], mesh.shape["tm"]
        self.bits, self.tm_bits = self.dp.bit_length() - 1, self.tm.bit_length() - 1
        self.top = self.bits + self.tm_bits - 1
        self.clips, self.group, self.frames = audio.shape
        self.half = self.group // 2
        self.cond = mel.shape[2]
        self.channels = start_weight.shape[1]
        self.layers, self.taps = input_weight.shape[:2]
        self.wide = 2 * self.channels
        self.rows = self.clips * self.frames
        self.all_rows = self.rows + self.clips * 2 * EDGE
        self.pad_rows = round_up(self.all_rows, LANES)
        self.own_ch = self.channels // self.dp
        self.own_cond = self.cond // self.dp
        self.width = self.wide // self.tm
        near = list(range(1, self.bits))
        far = near[::-1]
        along = list(range(self.bits, self.bits + self.tm_bits))
        routes = {
            "a": [0] + near + along,
            "b": [0] + far + along,
            "u": [0] + near[:1] + along + near[1:],
            "v": [0] + far[:1] + along + far[1:],
            "z": [0] + along + near,
            "w": [0] + along + far,
        }
        self.chunks = []
        for layer, part, ways in (
            (1, 0, "ab"),
            (1, 1, "wu"),
            (1, 2, "ba"),
            (1, COND, "wb"),
            (0, RES, "b"),
            (0, 0, "ub"),
            (0, 1, "ba"),
            (0, 2, "ab"),
            (0, COND, "bu"),
        ):
            high = self.part_rows(part)
            first = high if part == RES else round_up(high // 2, 16)
            columns = self.channels if part == RES else self.wide
            spans = [(0, first), (first, high - first)][: len(ways)]
            for (low, rows), way in zip(spans, ways):
                self.chunks.append((layer, part, low, rows, columns, routes[way]))

    def part_rows(self, part):
        return self.own_cond if part == COND else self.own_ch

    def open_bits(self, order, stage):
        done = set(order[: stage + 1])
        bits = [b for b in reversed(range(self.top + 1)) if b not in done]
        return [b for b in bits if b < self.bits], [b for b in bits if b >= self.bits]

    def pieced(self, order, stage):
        return any(b >= self.bits for b in order[: stage + 1])

    def recv_shape(self, chunk, stage):
        _, _, _, rows, columns, order = chunk
        height = round_up(rows, 16)
        open_dp, open_tm = self.open_bits(order, stage)
        if self.pieced(order, stage):
            return (2,) * len(open_tm + open_dp) + (height, self.width)
        return (2,) * len(open_dp) + (height, columns)


def kernel(plan, *refs):
    p = plan
    n_in, n_out = 8, 7
    (audio_h, mel_h, start_w, win_h, cond_h, res_h, last_h, end_w) = refs[:n_in]
    latent_o, audio_o, in_o, cond_o, res_o, small_o, end_o = refs[n_in : n_in + n_out]
    s = refs[n_in + n_out]
    me_dp, me_tm = lax.axis_index("dp"), lax.axis_index("tm")
    bit_of = [(me_dp // 2**b) % 2 for b in range(p.bits)]
    bit_of += [(me_tm // 2**b) % 2 for b in range(p.tm_bits)]
    ch, rows, all_rows, fr = p.channels, p.rows, p.all_rows, p.frames
    ext = fr + 2 * EDGE
    n_blocks = ch // BLOCK

    def partner(b):
        if b < p.bits:
            return {"dp": me_dp + (2**b) * (1 - 2 * bit_of[b]), "tm": me_tm}
        return {"dp": me_dp, "tm": me_tm + (2 ** (b - p.bits)) * (1 - 2 * bit_of[b])}

    def peer(step):
        return {"dp": me_dp, "tm": lax.rem(me_tm + step, p.tm)}

    def load(src, dst, index):
        copy = pltpu.make_async_copy(src, dst, s.load_sem.at[index])
        copy.start()
        return copy

    audio_load = load(audio_h, s.audio, 0)
    mel_loads = [
        load(mel_h.at[clip], s.mel.at[pl.ds(clip * fr, fr)], 1 + clip)
        for clip in range(p.clips)
    ]
    base = 1 + p.clips
    res_load = load(res_h, s.res, base + 2 * p.layers)
    last_load = load(last_h, s.last, base + 2 * p.layers + 1)
    weight_loads = []
    for layer in range(p.layers):
        at = base + 2 * layer
        weight_loads.append(
            [
                load(win_h.at[layer], s.win.at[layer], at),
                load(cond_h.at[layer], s.cond.at[layer], at + 1),
            ]
        )

    barrier = pltpu.get_barrier_semaphore()
    for b in range(p.bits):
        pl.semaphore_signal(barrier, 1, device_id=partner(b), device_id_type=MESH)
    for step in range(1, p.tm):
        pl.semaphore_signal(barrier, 1, device_id=peer(step), device_id_type=MESH)
    audio_load.wait()
    pl.semaphore_wait(barrier, p.bits + p.tm - 1)

    has_low, has_high = me_tm > 0, me_tm < p.tm - 1

    def halo_copies(slot):
        device = {"dp": me_dp, "tm": me_tm + 1 if slot == 0 else me_tm - 1}
        mel_at = fr - 2 * EDGE if slot == 0 else 0
        audio_at = fr - LANES if slot == 0 else 0
        return [
            pltpu.make_async_remote_copy(
                s.audio.at[:, :, pl.ds(audio_at, LANES)],
                s.audio_halo.at[slot],
                s.halo_send.at[slot, 0], s.halo_recv.at[slot, 0],
                device_id=device, device_id_type=MESH,
            ),
            pltpu.make_async_remote_copy(
                mel_h.at[:, pl.ds(mel_at, 2 * EDGE)],
                s.mel_halo.at[slot],
                s.halo_send.at[slot, 1], s.halo_recv.at[slot, 1],
                device_id=device, device_id_type=MESH,
            ),
        ]

    to_high, to_low = halo_copies(0), halo_copies(1)

    @pl.when(has_high)
    def _():
        for copy in to_high:
            copy.start()

    @pl.when(has_low)
    def _():
        for copy in to_low:
            copy.start()

    def halo_wait(index):
        @pl.when(has_low)
        def _():
            to_high[index].wait_recv()

        @pl.when(has_high)
        def _():
            to_low[index].wait_recv()

    def g_index(values):
        return tuple(values.get(b, slice(None)) for b in reversed(range(p.bits)))

    def cols_of(chunk_id, values):
        bits = p.tm_bits - 1 if narrow(chunk_id) else p.tm_bits
        owner = sum(values[p.bits + b] * 2**b for b in range(bits))
        return pl.ds(pl.multiple_of(owner * p.width, LANES), p.width)

    def narrow(chunk_id):
        return p.chunks[chunk_id][4] < p.wide

    def when_side(chunk_id, stage, side, run):
        if narrow(chunk_id) and p.chunks[chunk_id][5][stage] == p.top:
            pl.when(bit_of[p.top] == side)(run)
        else:
            run()

    def each(bits):
        for combo in itertools.product((0, 1), repeat=len(bits)):
            yield dict(zip(bits, combo))

    def pieces(chunk_id, stage):
        order = p.chunks[chunk_id][5]
        if not p.pieced(order, stage):
            return [{}]
        open_tm = p.open_bits(order, stage)[1]
        return [
            combo for combo in each(open_tm)
            if not (narrow(chunk_id) and combo.get(p.top, 0))
        ]

    def fixed_bits(chunk_id, stage):
        order = p.chunks[chunk_id][5]
        values = {b: bit_of[b] for b in order[:stage]}
        values[order[stage]] = 1 - bit_of[order[stage]]
        return values

    def terms(chunk_id, stage, values, where, cols):
        order = p.chunks[chunk_id][5]
        for done in range(stage):
            open_dp, open_tm = p.open_bits(order, done)
            at = tuple(values[b] for b in open_dp) + where
            if p.pieced(order, done):
                at = tuple(values[b] for b in open_tm) + at
            else:
                at += (cols,)
            yield s.recv[chunk_id][done][at]

    def add_blocks(chunk_id, stage):
        order = p.chunks[chunk_id][5]
        acc = s.grad[chunk_id]
        for piece in pieces(chunk_id, stage):
            for block in each(p.open_bits(order, stage)[0]):
                values = {**fixed_bits(chunk_id, stage), **piece, **block}
                split_cols = p.pieced(order, stage)
                cols = cols_of(chunk_id, values) if split_cols else slice(None)

                @pl.loop(0, acc.shape[-2] // 16)
                def _(r, values=values, cols=cols):
                    where = (pl.ds(pl.multiple_of(r * 16, 16), 16),)
                    total = acc[g_index(values) + where + (cols,)].astype(F32)
                    for term in terms(chunk_id, stage, values, where, cols):
                        total += term.astype(F32)
                    acc[g_index(values) + where + (cols,)] = total.astype(BF16)

    def copies(chunk_id, stage):
        order = p.chunks[chunk_id][5]
        out = []
        for slot, piece in enumerate(pieces(chunk_id, stage)):
            values = {**fixed_bits(chunk_id, stage), **piece}
            source, target = s.grad[chunk_id], s.recv[chunk_id][stage]
            if p.pieced(order, stage):
                source = source.at[g_index(values) + (slice(None), cols_of(chunk_id, values))]
                if piece:
                    target = target.at[tuple(piece.values())]
            else:
                source = source.at[g_index(values)]
            out.append(
                pltpu.make_async_remote_copy(
                    source, target,
                    s.grad_send.at[chunk_id, stage, slot],
                    s.grad_recv.at[chunk_id, stage, slot],
                    device_id=partner(order[stage]), device_id_type=MESH,
                )
            )
        return out

    def arrived(chunk_id, stage):
        def run():
            for copy in copies(chunk_id, stage):
                copy.wait_recv()

        when_side(chunk_id, stage, 0, run)

    sent = [0] * len(p.chunks)

    def send(chunk_id, stage):
        if stage >= len(p.chunks[chunk_id][5]):
            return
        sent[chunk_id] = stage + 1
        if stage:
            arrived(chunk_id, stage - 1)

        def run():
            if stage:
                add_blocks(chunk_id, stage)
            for copy in copies(chunk_id, stage):
                copy.start()

        when_side(chunk_id, stage, 1, run)

    def result_copy(chunk_id):
        layer, part, low, high, _, _ = p.chunks[chunk_id]
        span = pl.ds(low, high)
        if part == COND:
            target = cond_o.at[layer, span]
        elif part == RES:
            target = res_o.at[layer, span]
        else:
            target = in_o.at[layer, part, span]
        return pltpu.make_async_copy(s.result[chunk_id], target, s.out_sem.at[chunk_id])

    def finish(chunk_id):
        _, _, _, high, _, order = p.chunks[chunk_id]
        last = len(order) - 1
        values = {b: bit_of[b] for b in range(p.top + 1)}

        def run():
            for copy in copies(chunk_id, last):
                copy.wait_recv()
            where = (pl.ds(0, high),)
            cols = cols_of(chunk_id, values)
            total = s.grad[chunk_id][g_index(values) + where + (cols,)].astype(F32)
            for term in terms(chunk_id, last + 1, values, where, cols):
                total += term.astype(F32)
            s.result[chunk_id][...] = total
            result_copy(chunk_id).start()

        when_side(chunk_id, last, 0, run)

    def drain(chunk_id):
        for stage in range(len(p.chunks[chunk_id][5])):

            def run(stage=stage):
                for copy in copies(chunk_id, stage):
                    copy.wait_send()

            when_side(chunk_id, stage, 1, run)
        when_side(
            chunk_id, len(p.chunks[chunk_id][5]) - 1, 0, result_copy(chunk_id).wait
        )

    for clip in range(p.clips):
        mel_loads[clip].wait()
    s.mel_t[...] = jnp.transpose(s.mel[0:rows, :], (1, 0))
    res_load.wait()
    last_load.wait()
    end_cols = end_w[...]
    skips = [
        dot(end_cols, s.res[:, ch:], ((1,), (1,))),
        dot(end_cols, s.last[...], ((1,), (1,))),
    ]
    for layer in range(p.layers):
        coarse = skips[layer].astype(BF16)
        fine = skips[layer] - coarse.astype(F32)
        s.skip_w[layer] = jnp.concatenate(
            [coarse.astype(F32), fine], axis=0
        ).astype(BF16)
    lane_iota = lax.broadcasted_iota(jnp.int32, (p.group, LANES), 1)
    row_iota = lax.broadcasted_iota(jnp.int32, (p.group, LANES), 0)
    halo_wait(0)
    halo_lanes = p.pad_rows - rows
    blocks = [jnp.zeros((p.group, LANES), F32) for _ in range(halo_lanes // LANES)]
    lane_ok = [jnp.zeros((p.group, LANES), jnp.int32) for _ in range(halo_lanes // LANES)]
    low_ok = jnp.where(has_low, 1, 0)
    high_ok = jnp.where(has_high, 1, 0)
    for clip in range(p.clips):
        at = clip * 2 * EDGE
        block, lane = at // LANES, at % LANES
        for slot in range(2):
            first = lane + slot * EDGE
            inside = (lane_iota >= first) & (lane_iota < first + EDGE)
            ok = low_ok if slot == 0 else high_ok
            turned = pltpu.roll(s.audio_halo[slot, clip], (lane + EDGE) % LANES, 1)
            keep = inside & (jnp.broadcast_to(ok, inside.shape) > 0)
            blocks[block] = jnp.where(keep, turned, blocks[block])
            lane_ok[block] = jnp.where(keep, 1, lane_ok[block])
    audio_all = jnp.concatenate(
        [s.audio[clip] for clip in range(p.clips)] + blocks, axis=1
    )
    main_ok = jnp.ones((p.group, rows), jnp.int32)
    inside_clip = jnp.concatenate([main_ok] + lane_ok, axis=1) > 0
    group_rows = lax.broadcasted_iota(jnp.int32, (p.group, p.pad_rows), 0)
    first8 = jnp.where(group_rows < p.half, audio_all, 0.0)
    s.first[...] = first8[:, :rows]
    s.second[...] = pltpu.roll(audio_all, p.half, 0)
    start8 = s.start8
    start8[...] = jnp.zeros_like(start8)
    start8[0 : p.half] = start_w[...]
    first_cols = jnp.transpose(first8, (1, 0))
    for block in range(ch // LANES):
        cols = slice(block * LANES, (block + 1) * LANES)
        s.state[:, cols] = dot(
            first_cols[:all_rows], start8[:, cols], precision=HIGHEST
        )

    halo_wait(1)
    for clip in range(p.clips):
        low = s.mel_halo[0, clip].astype(F32)[EDGE:]
        high = s.mel_halo[1, clip].astype(F32)[:EDGE]
        low = jnp.where(jnp.broadcast_to(low_ok, low.shape) > 0, low, 0.0)
        high = jnp.where(jnp.broadcast_to(high_ok, high.shape) > 0, high, 0.0)
        s.mel[pl.ds(rows + clip * 2 * EDGE, 2 * EDGE)] = jnp.concatenate(
            [low, high], axis=0
        ).astype(BF16)

    def extended(ref, clip, cols):
        at = rows + clip * 2 * EDGE
        return jnp.concatenate(
            [
                ref[pl.ds(at, EDGE), cols],
                ref[pl.ds(clip * fr, fr), cols],
                ref[pl.ds(at + EDGE, EDGE), cols],
            ],
            axis=0,
        )

    def store_extended(ref, clip, cols, value):
        ref[pl.ds(clip * fr, fr), cols] = value[EDGE : EDGE + fr].astype(BF16)
        ref[pl.ds(rows + clip * 2 * EDGE, 2 * EDGE), cols] = jnp.concatenate(
            [value[:EDGE], value[EDGE + fr :]], axis=0
        ).astype(BF16)

    ext_iota = lax.broadcasted_iota(jnp.int32, (ext, LANES), 0)
    low_row = jnp.broadcast_to(me_tm == 0, (ext, LANES)) & (ext_iota < EDGE)
    high_row = jnp.broadcast_to(me_tm == p.tm - 1, (ext, LANES)) & (
        ext_iota >= EDGE + fr
    )
    outside = low_row | high_row

    def lanes_at(start):
        return pl.ds(pl.multiple_of(start, LANES), LANES)

    def block_at(start):
        return pl.ds(pl.multiple_of(start, BLOCK), BLOCK)

    def grad_block_at(start):
        return pl.ds(pl.multiple_of(start, GRAD_BLOCK), GRAD_BLOCK)

    def spread_state(layer):
        reach = 2**layer

        @pl.loop(0, ch // LANES)
        def _(block):
            for clip in range(p.clips):
                value = extended(s.state, clip, lanes_at(block * LANES))
                value = jnp.where(outside, 0.0, value)
                for tap in range(p.taps):
                    shift = ((1 - tap) * reach) % ext
                    moved = pltpu.roll(value, shift, 0) if shift else value
                    store_extended(
                        s.taps, clip, lanes_at(tap * ch + block * LANES), moved
                    )

        mid = p.taps // 2
        s.state_t[layer] = jnp.transpose(
            s.taps[0:rows, mid * ch : (mid + 1) * ch], (1, 0)
        )

    def gate(layer):
        @pl.loop(0, n_blocks)
        def _(n):
            pre = []
            for side in range(2):
                cols = block_at(side * ch + n * BLOCK)
                pre.append(
                    dot(s.taps[...], s.win[layer, :, cols])
                    + dot(s.mel[...], s.cond[layer, :, cols])
                )
            tangent = jnp.tanh(pre[0])
            switch = 0.5 * jnp.tanh(0.5 * pre[1]) + 0.5
            cols = block_at(n * BLOCK)
            s.tangent[layer, :, cols] = tangent
            s.switch[layer, :, cols] = switch
            s.gated[layer, 0:all_rows, cols] = (tangent * switch).astype(BF16)

    def gate_back(layer, taps):
        reach = 2**layer

        @pl.loop(0, ch // LANES)
        def _(block):
            cols = lanes_at(block * LANES)
            for clip in range(p.clips):
                up = extended(s.act, clip, cols)
                tangent = extended(s.tangent.at[layer], clip, cols)
                switch = extended(s.switch.at[layer], clip, cols)
                lift = jnp.where(outside, 0.0, up) * switch
                sides = (
                    lift * (1.0 - tangent * tangent),
                    lift * tangent * (1.0 - switch),
                )
                for side in range(2):
                    for tap in taps:
                        shift = ((tap - 1) * reach) % ext
                        moved = pltpu.roll(sides[side], shift, 0) if shift else sides[side]
                        store_extended(
                            s.back, clip,
                            lanes_at(tap * p.wide + side * ch + block * LANES), moved,
                        )

    def ids_of(layer, part):
        return [i for i, chunk in enumerate(p.chunks) if chunk[:2] == (layer, part)]

    def weight_grads(layer, part):
        ids = ids_of(layer, part)
        columns = p.chunks[ids[0]][4]
        high = p.part_rows(part)
        mid = p.taps // 2

        @pl.loop(0, columns // GRAD_BLOCK)
        def _(n):
            cols = grad_block_at(n * GRAD_BLOCK)
            if part == COND:
                left = s.mel_t[...]
                right = s.back[0:rows, grad_block_at(mid * p.wide + n * GRAD_BLOCK)]
            elif part == RES:
                left = s.gated_t[...]
                right = s.join[0:rows, cols]
            else:
                left = s.state_t[layer]
                right = s.back[0:rows, grad_block_at(part * p.wide + n * GRAD_BLOCK)]
            value = dot(left, right)
            for owner in range(p.dp):
                at = tuple((owner >> b) & 1 for b in reversed(range(p.bits)))
                for chunk_id in ids:
                    low, span = p.chunks[chunk_id][2:4]
                    start = owner * high + low
                    s.grad[chunk_id][at + (pl.ds(0, span), cols)] = value[
                        start : start + span
                    ].astype(BF16)

        for chunk_id in ids:
            send(chunk_id, 0)

    def state_grad(layer, accumulate, between):
        @pl.loop(0, n_blocks)
        def _(n):
            total = None
            for tap in range(p.taps):
                term = dot(
                    s.back[:, tap * p.wide : (tap + 1) * p.wide],
                    s.win[layer, block_at(tap * ch + n * BLOCK), :],
                    ((1,), (1,)),
                )
                total = term if total is None else total + term
            cols = block_at(n * BLOCK)
            if accumulate:
                total = total + s.state[:, cols]
            s.state[:, cols] = total
            pl.when(n == 0)(between)

    spread_state(0)
    for copy in weight_loads[0]:
        copy.wait()
    gate(0)
    @pl.loop(0, n_blocks)
    def _(n):
        cols = block_at(n * BLOCK)
        s.state[:, cols] = s.state[:, cols] + dot(
            s.gated[0, 0:all_rows, :], s.res[:, cols]
        )

    spread_state(1)
    for copy in weight_loads[1]:
        copy.wait()
    gate(1)

    out = None
    for layer in range(p.layers):
        term = dot(s.skip_w[layer], s.gated[layer], ((1,), (1,)))
        term = term[: p.group] + term[p.group :]
        out = term if out is None else out + term
    top = group_rows < p.half
    inside_top = top & inside_clip
    log_scale = jnp.where(inside_top, out, 0.0)
    shift_term = jnp.where(inside_top, pltpu.roll(out, p.half, 0), 0.0)
    growth = jnp.exp(log_scale)
    second = s.second[...]
    latent = growth * second + shift_term
    scale_inv = 1.0 / (p.clips * p.dp)
    upper = (latent * growth * second - 1.0) * scale_inv
    lower = pltpu.roll(jnp.where(top, latent, 0.0), p.half, 0) * scale_inv
    grad_out = jnp.where(inside_clip, jnp.where(top, upper, lower), 0.0)
    s.scaled[...] = (jnp.where(top, latent * growth, 0.0) * scale_inv)[:, :rows]
    for clip in range(p.clips):
        s.latent[clip] = latent[0 : p.half, clip * fr : (clip + 1) * fr]
    first = s.first[...]
    head = (latent * latent)[:, :rows] * 0.5 - log_scale[:, :rows]
    loss = jnp.sum(
        jnp.where(top[:, :rows], head, 0.0) + 0.5 * first * first, keepdims=True
    )
    s.loss[...] = jnp.broadcast_to(loss * scale_inv, s.loss.shape)
    grad_twice = jnp.concatenate([grad_out, grad_out], axis=0).astype(BF16)
    grad_b = grad_out.astype(BF16)
    for layer in range(p.layers):
        s.small[layer * p.group : (layer + 1) * p.group] = dot(
            grad_b[:, :rows], s.gated[layer, 0:rows, :]
        )
    s.grad_cols[...] = jnp.transpose(
        jnp.concatenate([grad_out, grad_out], axis=0), (1, 0)
    ).astype(BF16)

    s.act[...] = dot(s.grad_cols[0:all_rows], s.skip_w[1])
    gate_back(1, (1,))
    weight_grads(1, COND)
    weight_grads(1, 1)
    gate_back(1, (0, 2))
    send(6, 1)
    weight_grads(1, 0)
    send(2, 1)
    send(7, 1)
    send(3, 1)
    weight_grads(1, 2)

    def between1():
        send(1, 1)
        send(0, 1)

    state_grad(1, False, between1)
    send(5, 1)
    send(4, 1)
    @pl.loop(0, ch // LANES)
    def _(block):
        cols = lanes_at(block * LANES)
        for clip in range(p.clips):
            value = jnp.where(outside, 0.0, extended(s.state, clip, cols))
            store_extended(s.join, clip, cols, value)

    s.gated_t[...] = jnp.transpose(s.gated[0, 0:rows, :], (1, 0))
    weight_grads(0, RES)
    send(7, 2)
    send(3, 2)
    send(6, 2)
    @pl.loop(0, n_blocks)
    def _(n):
        cols = block_at(n * BLOCK)
        s.act[:, cols] = dot(
            s.join[...], s.res[cols, 0:ch], ((1,), (1,))
        ) + dot(s.grad_cols[0:all_rows], s.skip_w[0, :, cols])

    gate_back(0, (0, 1, 2))
    send(8, 1)
    send(2, 2)
    send(1, 2)
    send(0, 2)
    weight_grads(0, 0)
    send(3, 3)
    weight_grads(0, 1)
    send(5, 2)
    send(4, 2)
    weight_grads(0, COND)
    send(10, 1)
    send(7, 3)
    send(9, 1)
    weight_grads(0, 2)
    send(12, 1)
    send(1, 3)
    send(11, 1)
    send(6, 3)
    send(8, 2)

    def between0():
        send(15, 1)
        send(16, 1)
        send(0, 3)
        send(4, 3)
        send(13, 1)

    state_grad(0, True, between0)
    send(2, 3)
    send(14, 1)
    send(5, 3)
    small = s.small
    lead = 2 * p.group
    start_grad = dot(first, s.state[0:rows], precision=HIGHEST)
    start_rows = lax.broadcasted_iota(jnp.int32, start_grad.shape, 0)
    small[lead : lead + p.group] = jnp.where(
        start_rows == p.half, jnp.broadcast_to(s.loss[0:1, 0:1], start_grad.shape),
        start_grad,
    )
    s.small_tm[me_tm] = small[...]

    def small_tm(step):
        return pltpu.make_async_remote_copy(
            small, s.small_tm.at[me_tm],
            s.small_tm_send.at[step - 1], s.small_tm_recv.at[step - 1],
            device_id=peer(step), device_id_type=MESH,
        )

    def small_copy(stage):
        return pltpu.make_async_remote_copy(
            small, s.small_recv.at[stage],
            s.small_send_sem.at[stage], s.small_recv_sem.at[stage],
            device_id=partner(stage), device_id_type=MESH,
        )

    def small_step(stage):
        if stage:
            small_copy(stage - 1).wait()
            small[...] = small[...] + s.small_recv[stage - 1]
        else:
            for step in range(1, p.tm):
                small_tm(step).wait()
            total = s.small_tm[0]
            for at in range(1, p.tm):
                total += s.small_tm[at]
            small[...] = total
        if stage < p.bits:
            small_copy(stage).start()

    for step in range(1, p.tm):
        small_tm(step).start()
    send(3, 4)
    send(9, 2)
    first_back = dot(start8[...], s.state[0:rows], ((1,), (1,)), precision=HIGHEST)
    front = first_back + first * scale_inv
    back_rows = pltpu.roll(s.scaled[...], p.half, 0)
    audio_grad = jnp.where(group_rows[:, :rows] < p.half, front, back_rows)
    for clip in range(p.clips):
        s.audio_grad[clip] = audio_grad[:, clip * fr : (clip + 1) * fr]
    for chunk_id, stage in (
        (10, 2),
        (7, 4),
        (1, 4),
        (0, 4),
        (12, 2),
        (4, 4),
        (5, 4),
        (11, 2),
        (8, 3),
    ):
        send(chunk_id, stage)
    small_step(0)
    for chunk_id, stage in (
        (9, 3),
        (6, 4),
        (16, 2),
        (8, 4),
        (15, 2),
        (13, 2),
        (2, 4),
        (9, 4),
    ):
        send(chunk_id, stage)
    small_step(1)
    for chunk_id, stage in (
        (10, 3),
        (16, 3),
        (11, 3),
        (14, 2),
        (10, 4),
        (12, 3),
        (15, 3),
        (16, 4),
    ):
        send(chunk_id, stage)
    small_step(2)
    for chunk_id, stage in (
        (13, 3),
        (11, 4),
        (14, 3),
        (12, 4),
        (15, 4),
        (13, 4),
        (14, 4),
    ):
        send(chunk_id, stage)
    for stage in range(p.top + 1):
        for chunk_id in range(len(p.chunks)):
            if sent[chunk_id] == stage:
                send(chunk_id, stage)
    for stage in range(3, p.bits + 1):
        small_step(stage)

    total = small[...]
    m_first, m_last = total[: p.group], total[p.group : lead]
    end_t = None
    for m, w in ((m_first, s.res[:, ch:]), (m_last, s.last[...])):
        for term in split(m):
            part = dot(term, w)
            end_t = part if end_t is None else end_t + part
    s.end_t[...] = end_t
    others = [
        pltpu.make_async_copy(source, target, s.out_sem.at[len(p.chunks) + at])
        for at, (source, target) in enumerate(
            (
                (s.latent, latent_o), (s.audio_grad, audio_o), (small, small_o),
                (s.end_t, end_o),
            )
        )
    ]
    for copy in others:
        copy.start()

    for chunk_id in range(len(p.chunks)):
        finish(chunk_id)

    for chunk_id in range(len(p.chunks)):
        drain(chunk_id)
    for copy in others:
        copy.wait()

    @pl.when(has_high)
    def _():
        for copy in to_high:
            copy.wait_send()

    @pl.when(has_low)
    def _():
        for copy in to_low:
            copy.wait_send()


def split(value):
    coarse = value.astype(BF16)
    return coarse, (value - coarse.astype(F32)).astype(BF16)


def outputs_kernel(plan, *refs):
    p = plan
    held, end_w = refs[:7], refs[7]
    (
        latent_o, audio_o, loss_o, in_o, cond_o, res_o, last_o, end_o, start_o
    ) = refs[8:17]
    latent_s, audio_s, in_s, cond_s, res_s, small_s, end_s = refs[17:24]
    skip, last_s, load_sem, store_sem = refs[24:]
    me_dp, me_tm = lax.axis_index("dp"), lax.axis_index("tm")
    lead = 2 * p.group
    loads = [
        pltpu.make_async_copy(source, target, load_sem.at[at])
        for at, (source, target) in enumerate(zip(held, refs[17:24]))
    ]
    for at in (5, 2, 3, 4, 1, 0, 6):
        loads[at].start()
    stores = [
        pltpu.make_async_copy(source, target, store_sem.at[at])
        for at, (source, target) in enumerate(
            (
                (last_s, last_o), (in_s, in_o), (cond_s, cond_o), (audio_s, audio_o),
                (latent_s, latent_o), (end_s, end_o),
            )
        )
    ]
    loads[5].wait()
    end_rows = end_w[...]

    def spread(at, out_ref):
        m_cols = jnp.transpose(small_s[at : at + p.group], (1, 0))
        coarse, fine = split(m_cols)
        out_ref[...] = dot(coarse, end_rows) + dot(fine, end_rows)

    spread(p.group, last_s)
    stores[0].start()
    for load_at, store_at in ((2, 1), (3, 2), (1, 3), (0, 4), (6, 5)):
        loads[load_at].wait()
        stores[store_at].start()
    loss_o[...] = small_s[lead + p.half : lead + p.half + 1, 0:1]
    start_o[...] = small_s[lead : lead + p.half]
    loads[4].wait()
    res_owners = p.channels // p.width

    @pl.when(me_tm < res_owners)
    def _():
        res_o[...] = res_s[...]

    @pl.when(me_tm >= res_owners)
    def _():
        spread(0, skip)
        cols = pl.ds(pl.multiple_of((me_tm - res_owners) * p.width, LANES), p.width)
        at = pl.ds(pl.multiple_of(me_dp * p.own_ch, p.own_ch), p.own_ch)
        res_o[0] = skip[at, cols]

    for copy in stores:
        copy.wait()


def solution(mesh):
    def shards(
        audio, mel_frames, start_weight, input_weight, cond_weight, res_weight,
        last_weight, end_weight,
    ):
        p = Plan(mesh, audio, mel_frames, start_weight, input_weight)
        ch, wide, dp = p.channels, p.wide, p.dp
        vmem, anywhere = pltpu.VMEM, pl.BlockSpec(memory_space=pl.ANY)
        inside = pl.BlockSpec(memory_space=pltpu.VMEM)
        n_chunks = len(p.chunks)
        sem = pltpu.SemaphoreType.DMA
        scratch = dict(
            audio=vmem(audio.shape, F32),
            audio_halo=vmem((2, p.clips, p.group, LANES), F32),
            mel=vmem((p.all_rows, p.cond), BF16),
            mel_halo=vmem((2, p.clips, 2 * EDGE, p.cond), BF16),
            mel_t=vmem((p.cond, p.rows), BF16),
            win=vmem((p.layers, p.taps * ch, wide), BF16),
            cond=vmem((p.layers, p.cond, wide), BF16),
            res=vmem((ch, wide), BF16),
            last=vmem((ch, ch), BF16),
            first=vmem((p.group, p.rows), F32),
            second=vmem((p.group, p.pad_rows), F32),
            scaled=vmem((p.group, p.rows), F32),
            start8=vmem((p.group, ch), F32),
            loss=vmem((p.group, LANES), F32),
            state=vmem((p.all_rows, ch), F32),
            act=vmem((p.all_rows, ch), F32),
            taps=vmem((p.all_rows, p.taps * ch), BF16),
            state_t=vmem((p.layers, ch, p.rows), BF16),
            tangent=vmem((p.layers, p.all_rows, ch), F32),
            switch=vmem((p.layers, p.all_rows, ch), F32),
            gated=vmem((p.layers, p.pad_rows, ch), BF16),
            skip_w=vmem((p.layers, 2 * p.group, ch), BF16),
            grad_cols=vmem((p.pad_rows, 2 * p.group), BF16),
            join=vmem((p.all_rows, ch), BF16),
            gated_t=vmem((ch, p.rows), BF16),
            back=vmem((p.all_rows, p.taps * wide), BF16),
            small=vmem((3 * p.group, ch), F32),
            small_recv=vmem((p.bits, 3 * p.group, ch), F32),
            small_tm=vmem((p.tm, 3 * p.group, ch), F32),
            grad=[
                vmem((2,) * p.bits + p.recv_shape(chunk, 0)[-2:], BF16)
                for chunk in p.chunks
            ],
            recv=[
                [vmem(p.recv_shape(chunk, stage), BF16) for stage in range(p.top + 1)]
                for chunk in p.chunks
            ],
            load_sem=sem((3 + p.clips + 2 * p.layers,)),
            halo_send=sem((2, 2)),
            halo_recv=sem((2, 2)),
            grad_send=sem((n_chunks, p.top + 1, p.tm // 2)),
            grad_recv=sem((n_chunks, p.top + 1, p.tm // 2)),
            result=[vmem((chunk[3], p.width), F32) for chunk in p.chunks],
            latent=vmem((p.clips, p.half, p.frames), F32),
            audio_grad=vmem(audio.shape, F32),
            end_t=vmem((p.group, ch), F32),
            out_sem=sem((n_chunks + 4,)),
            small_send_sem=sem((p.bits,)),
            small_recv_sem=sem((p.bits,)),
            small_tm_send=sem((p.tm - 1,)),
            small_tm_recv=sem((p.tm - 1,)),
        )
        leaves, tree = jax.tree.flatten(scratch)

        def entry(*refs):
            fixed = 8 + 7
            names = types.SimpleNamespace(**jax.tree.unflatten(tree, refs[fixed:]))
            kernel(p, *refs[:fixed], names)

        shape = jax.ShapeDtypeStruct
        latent = shape((p.clips, p.half, p.frames), F32)
        audio_grad = shape(audio.shape, F32)
        in_grad = shape((p.layers, p.taps, p.own_ch, p.width), F32)
        cond_grad = shape((p.layers, p.own_cond, p.width), F32)
        res_grad = shape((p.layers - 1, p.own_ch, p.width), F32)
        end_grad = shape((p.group, ch), F32)
        end_t = end_weight.T
        held = pl.pallas_call(
            entry,
            out_shape=[
                latent, audio_grad, in_grad, cond_grad, res_grad,
                shape((3 * p.group, ch), F32), end_grad,
            ],
            in_specs=[
                anywhere, anywhere, inside, anywhere, anywhere, anywhere, anywhere, inside
            ],
            out_specs=[anywhere] * 7,
            scratch_shapes=leaves,
            compiler_params=pltpu.CompilerParams(
                collective_id=0, has_side_effects=True,
                vmem_limit_bytes=67_043_328,
            ),
            name="coupling_step",
        )(
            audio,
            mel_frames,
            start_weight,
            input_weight.reshape(p.layers, p.taps * ch, wide),
            cond_weight,
            res_weight.reshape(ch, wide),
            last_weight,
            end_t,
        )
        outs = pl.pallas_call(
            lambda *refs: outputs_kernel(p, *refs),
            out_shape=[
                latent, audio_grad, shape((1, 1), F32), in_grad, cond_grad, res_grad,
                shape(last_weight.shape, F32), end_grad, shape(start_weight.shape, F32),
            ],
            in_specs=[anywhere] * 7 + [inside],
            out_specs=[
                anywhere, anywhere, inside, anywhere, anywhere, inside, anywhere, anywhere,
                inside,
            ],
            scratch_shapes=[vmem(leaf.shape, F32) for leaf in held]
            + [vmem((ch, ch), F32)] * 2
            + [sem((7,)), sem((6,))],
            name="coupling_outputs",
        )(*held, end_t)
        outs = list(outs)
        outs[2] = outs[2].reshape(())
        outs[7] = outs[7].T
        return tuple(outs)

    return jax.shard_map(
        shards,
        mesh=mesh,
        in_specs=(P("dp", None, "tm"), P("dp", "tm", None), P(), P(), P(), P(), P(), P()),
        out_specs=(
            P("dp", None, "tm"),
            P("dp", None, "tm"),
            P(),
            P(None, None, "dp", "tm"),
            P(None, "dp", "tm"),
            P(None, "dp", "tm"),
            P(),
            P(),
            P(),
        ),
        check_vma=False,
    )
```

```python
import itertools
import types

import jax
import jax.numpy as jnp
from jax import lax
from jax.experimental import pallas as pl
from jax.experimental.pallas import tpu as pltpu
from jax.sharding import PartitionSpec as P

F32 = jnp.float32
BF16 = jnp.bfloat16
HIGHEST = lax.Precision.HIGHEST
MESH = pl.DeviceIdType.MESH


EDGE = 8
BLOCK = 256
GRAD_BLOCK = 512
LANES = 128
COND, RES = -1, -2


def dot(a, b, dims=((1,), (0,)), precision=None):
    return lax.dot_general(
        a, b, (dims, ((), ())), precision=precision, preferred_element_type=F32
    )


def round_up(value, unit):
    return -(-value // unit) * unit


class Plan:
    def __init__(self, mesh, audio, mel, start_weight, input_weight):
        self.dp, self.tm = mesh.shape["dp"], mesh.shape["tm"]
        self.bits, self.tm_bits = self.dp.bit_length() - 1, self.tm.bit_length() - 1
        self.top = self.bits + self.tm_bits - 1
        self.clips, self.group, self.frames = audio.shape
        self.half = self.group // 2
        self.cond = mel.shape[2]
        self.channels = start_weight.shape[1]
        self.layers, self.taps = input_weight.shape[:2]
        self.wide = 2 * self.channels
        self.rows = self.clips * self.frames
        self.all_rows = self.rows + self.clips * 2 * EDGE
        self.pad_rows = round_up(self.all_rows, LANES)
        self.own_ch = self.channels // self.dp
        self.own_cond = self.cond // self.dp
        self.width = self.wide // self.tm
        near = list(range(1, self.bits))
        far = near[::-1]
        along = list(range(self.bits, self.bits + self.tm_bits))
        routes = {
            "a": [0] + near + along,
            "b": [0] + far + along,
            "u": [0] + near[:1] + along + near[1:],
            "v": [0] + far[:1] + along + far[1:],
            "z": [0] + along + near,
            "w": [0] + along + far,
        }
        self.chunks = []
        for layer, part, ways in (
            (1, 0, "ab"),
            (1, 1, "wu"),
            (1, 2, "ba"),
            (1, COND, "wb"),
            (0, RES, "b"),
            (0, 0, "ub"),
            (0, 1, "ba"),
            (0, 2, "ab"),
            (0, COND, "bu"),
        ):
            high = self.part_rows(part)
            first = high if part == RES else round_up(high // 2, 16)
            columns = self.channels if part == RES else self.wide
            spans = [(0, first), (first, high - first)][: len(ways)]
            for (low, rows), way in zip(spans, ways):
                self.chunks.append((layer, part, low, rows, columns, routes[way]))

    def part_rows(self, part):
        return self.own_cond if part == COND else self.own_ch

    def open_bits(self, order, stage):
        done = set(order[: stage + 1])
        bits = [b for b in reversed(range(self.top + 1)) if b not in done]
        return [b for b in bits if b < self.bits], [b for b in bits if b >= self.bits]

    def pieced(self, order, stage):
        return any(b >= self.bits for b in order[: stage + 1])

    def recv_shape(self, chunk, stage):
        _, _, _, rows, columns, order = chunk
        height = round_up(rows, 16)
        open_dp, open_tm = self.open_bits(order, stage)
        if self.pieced(order, stage):
            return (2,) * len(open_tm + open_dp) + (height, self.width)
        return (2,) * len(open_dp) + (height, columns)


def kernel(plan, *refs):
    p = plan
    n_in, n_out = 8, 7
    (audio_h, mel_h, start_w, win_h, cond_h, res_h, last_h, end_w) = refs[:n_in]
    latent_o, audio_o, in_o, cond_o, res_o, small_o, end_o = refs[n_in : n_in + n_out]
    s = refs[n_in + n_out]
    me_dp, me_tm = lax.axis_index("dp"), lax.axis_index("tm")
    bit_of = [(me_dp // 2**b) % 2 for b in range(p.bits)]
    bit_of += [(me_tm // 2**b) % 2 for b in range(p.tm_bits)]
    ch, rows, all_rows, fr = p.channels, p.rows, p.all_rows, p.frames
    ext = fr + 2 * EDGE
    n_blocks = ch // BLOCK

    def partner(b):
        if b < p.bits:
            return {"dp": me_dp + (2**b) * (1 - 2 * bit_of[b]), "tm": me_tm}
        return {"dp": me_dp, "tm": me_tm + (2 ** (b - p.bits)) * (1 - 2 * bit_of[b])}

    def peer(step):
        return {"dp": me_dp, "tm": lax.rem(me_tm + step, p.tm)}

    def load(src, dst, index):
        copy = pltpu.make_async_copy(src, dst, s.load_sem.at[index])
        copy.start()
        return copy

    audio_load = load(audio_h, s.audio, 0)
    mel_loads = [
        load(mel_h.at[clip], s.mel.at[pl.ds(clip * fr, fr)], 1 + clip)
        for clip in range(p.clips)
    ]
    base = 1 + p.clips
    res_load = load(res_h, s.res, base + 2 * p.layers)
    last_load = load(last_h, s.last, base + 2 * p.layers + 1)
    weight_loads = []
    for layer in range(p.layers):
        at = base + 2 * layer
        weight_loads.append(
            [
                load(win_h.at[layer], s.win.at[layer], at),
                load(cond_h.at[layer], s.cond.at[layer], at + 1),
            ]
        )

    barrier = pltpu.get_barrier_semaphore()
    for b in range(p.bits):
        pl.semaphore_signal(barrier, 1, device_id=partner(b), device_id_type=MESH)
    for step in range(1, p.tm):
        pl.semaphore_signal(barrier, 1, device_id=peer(step), device_id_type=MESH)
    audio_load.wait()
    pl.semaphore_wait(barrier, p.bits + p.tm - 1)

    has_low, has_high = me_tm > 0, me_tm < p.tm - 1

    def halo_copies(slot):
        device = {"dp": me_dp, "tm": me_tm + 1 if slot == 0 else me_tm - 1}
        mel_at = fr - 2 * EDGE if slot == 0 else 0
        audio_at = fr - LANES if slot == 0 else 0
        return [
            pltpu.make_async_remote_copy(
                s.audio.at[:, :, pl.ds(audio_at, LANES)],
                s.audio_halo.at[slot],
                s.halo_send.at[slot, 0], s.halo_recv.at[slot, 0],
                device_id=device, device_id_type=MESH,
            ),
            pltpu.make_async_remote_copy(
                mel_h.at[:, pl.ds(mel_at, 2 * EDGE)],
                s.mel_halo.at[slot],
                s.halo_send.at[slot, 1], s.halo_recv.at[slot, 1],
                device_id=device, device_id_type=MESH,
            ),
        ]

    to_high, to_low = halo_copies(0), halo_copies(1)

    @pl.when(has_high)
    def _():
        for copy in to_high:
            copy.start()

    @pl.when(has_low)
    def _():
        for copy in to_low:
            copy.start()

    def halo_wait(index):
        @pl.when(has_low)
        def _():
            to_high[index].wait_recv()

        @pl.when(has_high)
        def _():
            to_low[index].wait_recv()

    def g_index(values):
        return tuple(values.get(b, slice(None)) for b in reversed(range(p.bits)))

    def cols_of(chunk_id, values):
        bits = p.tm_bits - 1 if narrow(chunk_id) else p.tm_bits
        owner = sum(values[p.bits + b] * 2**b for b in range(bits))
        return pl.ds(pl.multiple_of(owner * p.width, LANES), p.width)

    def narrow(chunk_id):
        return p.chunks[chunk_id][4] < p.wide

    def when_side(chunk_id, stage, side, run):
        if narrow(chunk_id) and p.chunks[chunk_id][5][stage] == p.top:
            pl.when(bit_of[p.top] == side)(run)
        else:
            run()

    def each(bits):
        for combo in itertools.product((0, 1), repeat=len(bits)):
            yield dict(zip(bits, combo))

    def pieces(chunk_id, stage):
        order = p.chunks[chunk_id][5]
        if not p.pieced(order, stage):
            return [{}]
        open_tm = p.open_bits(order, stage)[1]
        return [
            combo for combo in each(open_tm)
            if not (narrow(chunk_id) and combo.get(p.top, 0))
        ]

    def fixed_bits(chunk_id, stage):
        order = p.chunks[chunk_id][5]
        values = {b: bit_of[b] for b in order[:stage]}
        values[order[stage]] = 1 - bit_of[order[stage]]
        return values

    def terms(chunk_id, stage, values, where, cols):
        order = p.chunks[chunk_id][5]
        for done in range(stage):
            open_dp, open_tm = p.open_bits(order, done)
            at = tuple(values[b] for b in open_dp) + where
            if p.pieced(order, done):
                at = tuple(values[b] for b in open_tm) + at
            else:
                at += (cols,)
            yield s.recv[chunk_id][done][at]

    def add_blocks(chunk_id, stage):
        order = p.chunks[chunk_id][5]
        acc = s.grad[chunk_id]
        for piece in pieces(chunk_id, stage):
            for block in each(p.open_bits(order, stage)[0]):
                values = {**fixed_bits(chunk_id, stage), **piece, **block}
                split_cols = p.pieced(order, stage)
                cols = cols_of(chunk_id, values) if split_cols else slice(None)

                @pl.loop(0, acc.shape[-2] // 16)
                def _(r, values=values, cols=cols):
                    where = (pl.ds(pl.multiple_of(r * 16, 16), 16),)
                    total = acc[g_index(values) + where + (cols,)].astype(F32)
                    for term in terms(chunk_id, stage, values, where, cols):
                        total += term.astype(F32)
                    acc[g_index(values) + where + (cols,)] = total.astype(BF16)

    def copies(chunk_id, stage):
        order = p.chunks[chunk_id][5]
        out = []
        before = sum(2 ** len(p.open_bits(order, k)[1]) if p.pieced(order, k) else 1 for k in range(stage))
        for slot, piece in enumerate(pieces(chunk_id, stage)):
            values = {**fixed_bits(chunk_id, stage), **piece}
            source, target = s.grad[chunk_id], s.recv[chunk_id][stage]
            if p.pieced(order, stage):
                source = source.at[g_index(values) + (slice(None), cols_of(chunk_id, values))]
                if piece:
                    target = target.at[tuple(piece.values())]
            else:
                source = source.at[g_index(values)]
            out.append(
                pltpu.make_async_remote_copy(
                    source, target,
                    s.grad_send.at[chunk_id, slot],
                    s.grad_recv.at[chunk_id, before + slot],
                    device_id=partner(order[stage]), device_id_type=MESH,
                )
            )
        return out

    def arrived(chunk_id, stage):
        def run():
            for copy in copies(chunk_id, stage):
                copy.wait_recv()

        when_side(chunk_id, stage, 0, run)

    def left(chunk_id, stage):
        def run():
            for copy in copies(chunk_id, stage):
                copy.wait_send()

        when_side(chunk_id, stage, 1, run)

    sent = [0] * len(p.chunks)

    def send(chunk_id, stage):
        if stage >= len(p.chunks[chunk_id][5]):
            return
        sent[chunk_id] = stage + 1
        if stage:
            arrived(chunk_id, stage - 1)
            left(chunk_id, stage - 1)

        def run():
            if stage:
                add_blocks(chunk_id, stage)
            for copy in copies(chunk_id, stage):
                copy.start()

        when_side(chunk_id, stage, 1, run)

    def result_copy(chunk_id):
        layer, part, low, high, _, _ = p.chunks[chunk_id]
        span = pl.ds(low, high)
        if part == COND:
            target = cond_o.at[layer, span]
        elif part == RES:
            target = res_o.at[layer, span]
        else:
            target = in_o.at[layer, part, span]
        return pltpu.make_async_copy(s.result[chunk_id], target, s.out_sem.at[chunk_id])

    def finish(chunk_id):
        _, _, _, high, _, order = p.chunks[chunk_id]
        last = len(order) - 1
        values = {b: bit_of[b] for b in range(p.top + 1)}

        def run():
            for copy in copies(chunk_id, last):
                copy.wait_recv()
            where = (pl.ds(0, high),)
            cols = cols_of(chunk_id, values)
            total = s.grad[chunk_id][g_index(values) + where + (cols,)].astype(F32)
            for term in terms(chunk_id, last + 1, values, where, cols):
                total += term.astype(F32)
            s.result[chunk_id][...] = total
            result_copy(chunk_id).start()

        when_side(chunk_id, last, 0, run)

    def drain(chunk_id):
        left(chunk_id, len(p.chunks[chunk_id][5]) - 1)
        when_side(
            chunk_id, len(p.chunks[chunk_id][5]) - 1, 0, result_copy(chunk_id).wait
        )

    for clip in range(p.clips):
        mel_loads[clip].wait()
    s.mel_t[...] = jnp.transpose(s.mel[0:rows, :], (1, 0))
    res_load.wait()
    last_load.wait()
    end_cols = end_w[...]
    skips = [
        dot(end_cols, s.res[:, ch:], ((1,), (1,))),
        dot(end_cols, s.last[...], ((1,), (1,))),
    ]
    for layer in range(p.layers):
        coarse = skips[layer].astype(BF16)
        fine = skips[layer] - coarse.astype(F32)
        s.skip_w[layer] = jnp.concatenate(
            [coarse.astype(F32), fine], axis=0
        ).astype(BF16)
    lane_iota = lax.broadcasted_iota(jnp.int32, (p.group, LANES), 1)
    row_iota = lax.broadcasted_iota(jnp.int32, (p.group, LANES), 0)
    halo_wait(0)
    halo_lanes = p.pad_rows - rows
    blocks = [jnp.zeros((p.group, LANES), F32) for _ in range(halo_lanes // LANES)]
    lane_ok = [jnp.zeros((p.group, LANES), jnp.int32) for _ in range(halo_lanes // LANES)]
    low_ok = jnp.where(has_low, 1, 0)
    high_ok = jnp.where(has_high, 1, 0)
    for clip in range(p.clips):
        at = clip * 2 * EDGE
        block, lane = at // LANES, at % LANES
        for slot in range(2):
            first = lane + slot * EDGE
            inside = (lane_iota >= first) & (lane_iota < first + EDGE)
            ok = low_ok if slot == 0 else high_ok
            turned = pltpu.roll(s.audio_halo[slot, clip], (lane + EDGE) % LANES, 1)
            keep = inside & (jnp.broadcast_to(ok, inside.shape) > 0)
            blocks[block] = jnp.where(keep, turned, blocks[block])
            lane_ok[block] = jnp.where(keep, 1, lane_ok[block])
    audio_all = jnp.concatenate(
        [s.audio[clip] for clip in range(p.clips)] + blocks, axis=1
    )
    main_ok = jnp.ones((p.group, rows), jnp.int32)
    inside_clip = jnp.concatenate([main_ok] + lane_ok, axis=1) > 0
    group_rows = lax.broadcasted_iota(jnp.int32, (p.group, p.pad_rows), 0)
    first8 = jnp.where(group_rows < p.half, audio_all, 0.0)
    s.first[...] = first8[:, :rows]
    s.second[...] = pltpu.roll(audio_all, p.half, 0)
    start8 = s.start8
    start8[...] = jnp.zeros_like(start8)
    start8[0 : p.half] = start_w[...]
    first_cols = jnp.transpose(first8, (1, 0))
    for block in range(ch // LANES):
        cols = slice(block * LANES, (block + 1) * LANES)
        s.state[:, cols] = dot(
            first_cols[:all_rows], start8[:, cols], precision=HIGHEST
        )

    halo_wait(1)
    for clip in range(p.clips):
        low = s.mel_halo[0, clip].astype(F32)[EDGE:]
        high = s.mel_halo[1, clip].astype(F32)[:EDGE]
        low = jnp.where(jnp.broadcast_to(low_ok, low.shape) > 0, low, 0.0)
        high = jnp.where(jnp.broadcast_to(high_ok, high.shape) > 0, high, 0.0)
        s.mel[pl.ds(rows + clip * 2 * EDGE, 2 * EDGE)] = jnp.concatenate(
            [low, high], axis=0
        ).astype(BF16)

    def extended(ref, clip, cols):
        at = rows + clip * 2 * EDGE
        return jnp.concatenate(
            [
                ref[pl.ds(at, EDGE), cols],
                ref[pl.ds(clip * fr, fr), cols],
                ref[pl.ds(at + EDGE, EDGE), cols],
            ],
            axis=0,
        )

    def store_extended(ref, clip, cols, value):
        ref[pl.ds(clip * fr, fr), cols] = value[EDGE : EDGE + fr].astype(BF16)
        ref[pl.ds(rows + clip * 2 * EDGE, 2 * EDGE), cols] = jnp.concatenate(
            [value[:EDGE], value[EDGE + fr :]], axis=0
        ).astype(BF16)

    ext_iota = lax.broadcasted_iota(jnp.int32, (ext, LANES), 0)
    low_row = jnp.broadcast_to(me_tm == 0, (ext, LANES)) & (ext_iota < EDGE)
    high_row = jnp.broadcast_to(me_tm == p.tm - 1, (ext, LANES)) & (
        ext_iota >= EDGE + fr
    )
    outside = low_row | high_row

    def lanes_at(start):
        return pl.ds(pl.multiple_of(start, LANES), LANES)

    def block_at(start):
        return pl.ds(pl.multiple_of(start, BLOCK), BLOCK)

    def grad_block_at(start):
        return pl.ds(pl.multiple_of(start, GRAD_BLOCK), GRAD_BLOCK)

    def spread_state(layer):
        reach = 2**layer

        @pl.loop(0, ch // LANES)
        def _(block):
            for clip in range(p.clips):
                value = extended(s.state, clip, lanes_at(block * LANES))
                value = jnp.where(outside, 0.0, value)
                for tap in range(p.taps):
                    shift = ((1 - tap) * reach) % ext
                    moved = pltpu.roll(value, shift, 0) if shift else value
                    store_extended(
                        s.taps, clip, lanes_at(tap * ch + block * LANES), moved
                    )

        mid = p.taps // 2
        s.state_t[layer] = jnp.transpose(
            s.taps[0:rows, mid * ch : (mid + 1) * ch], (1, 0)
        )

    def gate(layer):
        @pl.loop(0, n_blocks)
        def _(n):
            pre = []
            for side in range(2):
                cols = block_at(side * ch + n * BLOCK)
                pre.append(
                    dot(s.taps[...], s.win[layer, :, cols])
                    + dot(s.mel[...], s.cond[layer, :, cols])
                )
            tangent = jnp.tanh(pre[0])
            switch = 0.5 * jnp.tanh(0.5 * pre[1]) + 0.5
            cols = block_at(n * BLOCK)
            s.tangent[layer, :, cols] = tangent
            s.switch[layer, :, cols] = switch
            s.gated[layer, 0:all_rows, cols] = (tangent * switch).astype(BF16)

    def gate_back(layer, taps):
        reach = 2**layer

        @pl.loop(0, ch // LANES)
        def _(block):
            cols = lanes_at(block * LANES)
            for clip in range(p.clips):
                up = extended(s.act, clip, cols)
                tangent = extended(s.tangent.at[layer], clip, cols)
                switch = extended(s.switch.at[layer], clip, cols)
                lift = jnp.where(outside, 0.0, up) * switch
                sides = (
                    lift * (1.0 - tangent * tangent),
                    lift * tangent * (1.0 - switch),
                )
                for side in range(2):
                    for tap in taps:
                        shift = ((tap - 1) * reach) % ext
                        moved = pltpu.roll(sides[side], shift, 0) if shift else sides[side]
                        store_extended(
                            s.back, clip,
                            lanes_at(tap * p.wide + side * ch + block * LANES), moved,
                        )

    def ids_of(layer, part):
        return [i for i, chunk in enumerate(p.chunks) if chunk[:2] == (layer, part)]

    def weight_grads(layer, part):
        ids = ids_of(layer, part)
        columns = p.chunks[ids[0]][4]
        high = p.part_rows(part)
        mid = p.taps // 2

        @pl.loop(0, columns // GRAD_BLOCK)
        def _(n):
            cols = grad_block_at(n * GRAD_BLOCK)
            if part == COND:
                left = s.mel_t[...]
                right = s.back[0:rows, grad_block_at(mid * p.wide + n * GRAD_BLOCK)]
            elif part == RES:
                left = s.gated_t[...]
                right = s.join[0:rows, cols]
            else:
                left = s.state_t[layer]
                right = s.back[0:rows, grad_block_at(part * p.wide + n * GRAD_BLOCK)]
            value = dot(left, right)
            for owner in range(p.dp):
                at = tuple((owner >> b) & 1 for b in reversed(range(p.bits)))
                for chunk_id in ids:
                    low, span = p.chunks[chunk_id][2:4]
                    start = owner * high + low
                    s.grad[chunk_id][at + (pl.ds(0, span), cols)] = value[
                        start : start + span
                    ].astype(BF16)

        for chunk_id in ids:
            send(chunk_id, 0)

    def state_grad(layer, accumulate, between):
        @pl.loop(0, n_blocks)
        def _(n):
            total = None
            for tap in range(p.taps):
                term = dot(
                    s.back[:, tap * p.wide : (tap + 1) * p.wide],
                    s.win[layer, block_at(tap * ch + n * BLOCK), :],
                    ((1,), (1,)),
                )
                total = term if total is None else total + term
            cols = block_at(n * BLOCK)
            if accumulate:
                total = total + s.state[:, cols]
            s.state[:, cols] = total
            pl.when(n == 0)(between)

    spread_state(0)
    for copy in weight_loads[0]:
        copy.wait()
    gate(0)
    @pl.loop(0, n_blocks)
    def _(n):
        cols = block_at(n * BLOCK)
        s.state[:, cols] = s.state[:, cols] + dot(
            s.gated[0, 0:all_rows, :], s.res[:, cols]
        )

    spread_state(1)
    for copy in weight_loads[1]:
        copy.wait()
    gate(1)

    out = None
    for layer in range(p.layers):
        term = dot(s.skip_w[layer], s.gated[layer], ((1,), (1,)))
        term = term[: p.group] + term[p.group :]
        out = term if out is None else out + term
    top = group_rows < p.half
    inside_top = top & inside_clip
    log_scale = jnp.where(inside_top, out, 0.0)
    shift_term = jnp.where(inside_top, pltpu.roll(out, p.half, 0), 0.0)
    growth = jnp.exp(log_scale)
    second = s.second[...]
    latent = growth * second + shift_term
    scale_inv = 1.0 / (p.clips * p.dp)
    upper = (latent * growth * second - 1.0) * scale_inv
    lower = pltpu.roll(jnp.where(top, latent, 0.0), p.half, 0) * scale_inv
    grad_out = jnp.where(inside_clip, jnp.where(top, upper, lower), 0.0)
    s.scaled[...] = (jnp.where(top, latent * growth, 0.0) * scale_inv)[:, :rows]
    for clip in range(p.clips):
        s.latent[clip] = latent[0 : p.half, clip * fr : (clip + 1) * fr]
    first = s.first[...]
    head = (latent * latent)[:, :rows] * 0.5 - log_scale[:, :rows]
    loss = jnp.sum(
        jnp.where(top[:, :rows], head, 0.0) + 0.5 * first * first, keepdims=True
    )
    s.loss[...] = jnp.broadcast_to(loss * scale_inv, s.loss.shape)
    grad_twice = jnp.concatenate([grad_out, grad_out], axis=0).astype(BF16)
    grad_b = grad_out.astype(BF16)
    for layer in range(p.layers):
        s.small[layer * p.group : (layer + 1) * p.group] = dot(
            grad_b[:, :rows], s.gated[layer, 0:rows, :]
        )
    s.grad_cols[...] = jnp.transpose(
        jnp.concatenate([grad_out, grad_out], axis=0), (1, 0)
    ).astype(BF16)

    s.act[...] = dot(s.grad_cols[0:all_rows], s.skip_w[1])
    gate_back(1, (1,))
    weight_grads(1, COND)
    weight_grads(1, 1)
    gate_back(1, (0, 2))
    send(6, 1)
    weight_grads(1, 0)
    send(2, 1)
    send(7, 1)
    send(3, 1)
    weight_grads(1, 2)

    def between1():
        send(1, 1)
        send(0, 1)

    state_grad(1, False, between1)
    send(5, 1)
    send(4, 1)
    @pl.loop(0, ch // LANES)
    def _(block):
        cols = lanes_at(block * LANES)
        for clip in range(p.clips):
            value = jnp.where(outside, 0.0, extended(s.state, clip, cols))
            store_extended(s.join, clip, cols, value)

    s.gated_t[...] = jnp.transpose(s.gated[0, 0:rows, :], (1, 0))
    weight_grads(0, RES)
    send(7, 2)
    send(3, 2)
    send(6, 2)
    @pl.loop(0, n_blocks)
    def _(n):
        cols = block_at(n * BLOCK)
        s.act[:, cols] = dot(
            s.join[...], s.res[cols, 0:ch], ((1,), (1,))
        ) + dot(s.grad_cols[0:all_rows], s.skip_w[0, :, cols])

    gate_back(0, (0, 1, 2))
    send(8, 1)
    send(2, 2)
    send(1, 2)
    send(0, 2)
    weight_grads(0, 0)
    send(3, 3)
    weight_grads(0, 1)
    send(5, 2)
    send(4, 2)
    weight_grads(0, COND)
    send(10, 1)
    send(7, 3)
    send(9, 1)
    weight_grads(0, 2)
    send(12, 1)
    send(1, 3)
    send(11, 1)
    send(6, 3)
    send(8, 2)

    def between0():
        send(15, 1)
        send(16, 1)
        send(0, 3)
        send(4, 3)
        send(13, 1)

    state_grad(0, True, between0)
    send(2, 3)
    send(14, 1)
    send(5, 3)
    small = s.small
    lead = 2 * p.group
    start_grad = dot(first, s.state[0:rows], precision=HIGHEST)
    start_rows = lax.broadcasted_iota(jnp.int32, start_grad.shape, 0)
    small[lead : lead + p.group] = jnp.where(
        start_rows == p.half, jnp.broadcast_to(s.loss[0:1, 0:1], start_grad.shape),
        start_grad,
    )
    s.small_tm[me_tm] = small[...]

    def small_tm(step):
        return pltpu.make_async_remote_copy(
            small, s.small_tm.at[me_tm],
            s.small_tm_send.at[step - 1], s.small_tm_recv.at[step - 1],
            device_id=peer(step), device_id_type=MESH,
        )

    def small_copy(stage):
        return pltpu.make_async_remote_copy(
            small, s.small_recv.at[stage],
            s.small_send_sem.at[stage], s.small_recv_sem.at[stage],
            device_id=partner(stage), device_id_type=MESH,
        )

    def small_step(stage):
        if stage:
            small_copy(stage - 1).wait()
            small[...] = small[...] + s.small_recv[stage - 1]
        else:
            for step in range(1, p.tm):
                small_tm(step).wait()
            total = s.small_tm[0]
            for at in range(1, p.tm):
                total += s.small_tm[at]
            small[...] = total
        if stage < p.bits:
            small_copy(stage).start()

    for step in range(1, p.tm):
        small_tm(step).start()
    send(3, 4)
    send(9, 2)
    first_back = dot(start8[...], s.state[0:rows], ((1,), (1,)), precision=HIGHEST)
    front = first_back + first * scale_inv
    back_rows = pltpu.roll(s.scaled[...], p.half, 0)
    audio_grad = jnp.where(group_rows[:, :rows] < p.half, front, back_rows)
    for clip in range(p.clips):
        s.audio_grad[clip] = audio_grad[:, clip * fr : (clip + 1) * fr]
    for chunk_id, stage in (
        (10, 2),
        (7, 4),
        (1, 4),
        (0, 4),
        (12, 2),
        (4, 4),
        (5, 4),
        (11, 2),
        (8, 3),
    ):
        send(chunk_id, stage)
    small_step(0)
    for chunk_id, stage in (
        (9, 3),
        (6, 4),
        (16, 2),
        (8, 4),
        (15, 2),
        (13, 2),
        (2, 4),
        (9, 4),
    ):
        send(chunk_id, stage)
    small_step(1)
    for chunk_id, stage in (
        (10, 3),
        (16, 3),
        (11, 3),
        (14, 2),
        (10, 4),
        (12, 3),
        (15, 3),
        (16, 4),
    ):
        send(chunk_id, stage)
    small_step(2)
    for chunk_id, stage in (
        (13, 3),
        (11, 4),
        (14, 3),
        (12, 4),
        (15, 4),
        (13, 4),
        (14, 4),
    ):
        send(chunk_id, stage)
    for stage in range(p.top + 1):
        for chunk_id in range(len(p.chunks)):
            if sent[chunk_id] == stage:
                send(chunk_id, stage)
    for stage in range(3, p.bits + 1):
        small_step(stage)

    total = small[...]
    m_first, m_last = total[: p.group], total[p.group : lead]
    end_t = None
    for m, w in ((m_first, s.res[:, ch:]), (m_last, s.last[...])):
        for term in split(m):
            part = dot(term, w)
            end_t = part if end_t is None else end_t + part
    s.end_t[...] = end_t
    others = [
        pltpu.make_async_copy(source, target, s.out_sem.at[len(p.chunks) + at])
        for at, (source, target) in enumerate(
            (
                (s.latent, latent_o), (s.audio_grad, audio_o), (small, small_o),
                (s.end_t, end_o),
            )
        )
    ]
    for copy in others:
        copy.start()

    for chunk_id in range(len(p.chunks)):
        finish(chunk_id)

    for chunk_id in range(len(p.chunks)):
        drain(chunk_id)
    for copy in others:
        copy.wait()

    @pl.when(has_high)
    def _():
        for copy in to_high:
            copy.wait_send()

    @pl.when(has_low)
    def _():
        for copy in to_low:
            copy.wait_send()


def split(value):
    coarse = value.astype(BF16)
    return coarse, (value - coarse.astype(F32)).astype(BF16)


def outputs_kernel(plan, *refs):
    p = plan
    (latent_i, audio_i, in_i, cond_i, res_i, small_i, end_i, end_w) = refs[:8]
    (
        latent_o, audio_o, loss_o, in_o, cond_o, res_o, last_o, end_o, start_o, skip
    ) = refs[8:]
    me_dp, me_tm = lax.axis_index("dp"), lax.axis_index("tm")
    lead = 2 * p.group
    for source, target in (
        (latent_i, latent_o), (audio_i, audio_o), (in_i, in_o), (cond_i, cond_o),
        (end_i, end_o),
    ):
        target[...] = source[...]
    loss_o[...] = small_i[lead + p.half : lead + p.half + 1, 0:1]
    start_o[...] = small_i[lead : lead + p.half]
    end_rows = end_w[...]

    def spread(at, out_ref):
        m_cols = jnp.transpose(small_i[at : at + p.group], (1, 0))
        coarse, fine = split(m_cols)
        out_ref[...] = dot(coarse, end_rows) + dot(fine, end_rows)

    spread(p.group, last_o)
    res_owners = p.channels // p.width

    @pl.when(me_tm < res_owners)
    def _():
        res_o[...] = res_i[...]

    @pl.when(me_tm >= res_owners)
    def _():
        spread(0, skip)
        cols = pl.ds(pl.multiple_of((me_tm - res_owners) * p.width, LANES), p.width)
        at = pl.ds(pl.multiple_of(me_dp * p.own_ch, p.own_ch), p.own_ch)
        res_o[0] = skip[at, cols]


def solution(mesh):
    def shards(
        audio, mel_frames, start_weight, input_weight, cond_weight, res_weight,
        last_weight, end_weight,
    ):
        p = Plan(mesh, audio, mel_frames, start_weight, input_weight)
        ch, wide, dp = p.channels, p.wide, p.dp
        vmem, anywhere = pltpu.VMEM, pl.BlockSpec(memory_space=pl.ANY)
        inside = pl.BlockSpec(memory_space=pltpu.VMEM)
        n_chunks = len(p.chunks)
        sem = pltpu.SemaphoreType.DMA
        scratch = dict(
            audio=vmem(audio.shape, F32),
            audio_halo=vmem((2, p.clips, p.group, LANES), F32),
            mel=vmem((p.all_rows, p.cond), BF16),
            mel_halo=vmem((2, p.clips, 2 * EDGE, p.cond), BF16),
            mel_t=vmem((p.cond, p.rows), BF16),
            win=vmem((p.layers, p.taps * ch, wide), BF16),
            cond=vmem((p.layers, p.cond, wide), BF16),
            res=vmem((ch, wide), BF16),
            last=vmem((ch, ch), BF16),
            first=vmem((p.group, p.rows), F32),
            second=vmem((p.group, p.pad_rows), F32),
            scaled=vmem((p.group, p.rows), F32),
            start8=vmem((p.group, ch), F32),
            loss=vmem((p.group, LANES), F32),
            state=vmem((p.all_rows, ch), F32),
            act=vmem((p.all_rows, ch), F32),
            taps=vmem((p.all_rows, p.taps * ch), BF16),
            state_t=vmem((p.layers, ch, p.rows), BF16),
            tangent=vmem((p.layers, p.all_rows, ch), F32),
            switch=vmem((p.layers, p.all_rows, ch), F32),
            gated=vmem((p.layers, p.pad_rows, ch), BF16),
            skip_w=vmem((p.layers, 2 * p.group, ch), BF16),
            grad_cols=vmem((p.pad_rows, 2 * p.group), BF16),
            join=vmem((p.all_rows, ch), BF16),
            gated_t=vmem((ch, p.rows), BF16),
            back=vmem((p.all_rows, p.taps * wide), BF16),
            small=vmem((3 * p.group, ch), F32),
            small_recv=vmem((p.bits, 3 * p.group, ch), F32),
            small_tm=vmem((p.tm, 3 * p.group, ch), F32),
            grad=[
                vmem((2,) * p.bits + p.recv_shape(chunk, 0)[-2:], BF16)
                for chunk in p.chunks
            ],
            recv=[
                [vmem(p.recv_shape(chunk, stage), BF16) for stage in range(p.top + 1)]
                for chunk in p.chunks
            ],
            load_sem=sem((3 + p.clips + 2 * p.layers,)),
            halo_send=sem((2, 2)),
            halo_recv=sem((2, 2)),
            grad_send=sem((n_chunks, p.tm // 2)),
            grad_recv=sem((n_chunks, p.bits + p.tm - 1)),
            result=[vmem((chunk[3], p.width), F32) for chunk in p.chunks],
            latent=vmem((p.clips, p.half, p.frames), F32),
            audio_grad=vmem(audio.shape, F32),
            end_t=vmem((p.group, ch), F32),
            out_sem=sem((n_chunks + 4,)),
            small_send_sem=sem((p.bits,)),
            small_recv_sem=sem((p.bits,)),
            small_tm_send=sem((p.tm - 1,)),
            small_tm_recv=sem((p.tm - 1,)),
        )
        leaves, tree = jax.tree.flatten(scratch)

        def entry(*refs):
            fixed = 8 + 7
            names = types.SimpleNamespace(**jax.tree.unflatten(tree, refs[fixed:]))
            kernel(p, *refs[:fixed], names)

        shape = jax.ShapeDtypeStruct
        latent = shape((p.clips, p.half, p.frames), F32)
        audio_grad = shape(audio.shape, F32)
        in_grad = shape((p.layers, p.taps, p.own_ch, p.width), F32)
        cond_grad = shape((p.layers, p.own_cond, p.width), F32)
        res_grad = shape((p.layers - 1, p.own_ch, p.width), F32)
        end_grad = shape((p.group, ch), F32)
        end_t = end_weight.T
        held = pl.pallas_call(
            entry,
            out_shape=[
                latent, audio_grad, in_grad, cond_grad, res_grad,
                shape((3 * p.group, ch), F32), end_grad,
            ],
            in_specs=[
                anywhere, anywhere, inside, anywhere, anywhere, anywhere, anywhere, inside
            ],
            out_specs=[anywhere] * 7,
            scratch_shapes=leaves,
            compiler_params=pltpu.CompilerParams(
                collective_id=0, has_side_effects=True,
                vmem_limit_bytes=67_043_328,
            ),
            name="coupling_step",
        )(
            audio,
            mel_frames,
            start_weight,
            input_weight.reshape(p.layers, p.taps * ch, wide),
            cond_weight,
            res_weight.reshape(ch, wide),
            last_weight,
            end_t,
        )
        outs = pl.pallas_call(
            lambda *refs: outputs_kernel(p, *refs),
            out_shape=[
                latent, audio_grad, shape((1, 1), F32), in_grad, cond_grad, res_grad,
                shape(last_weight.shape, F32), end_grad, shape(start_weight.shape, F32),
            ],
            in_specs=[inside] * 8,
            out_specs=[inside] * 9,
            scratch_shapes=[vmem((ch, ch), F32)],
            name="coupling_outputs",
        )(*held, end_t)
        outs = list(outs)
        outs[2] = outs[2].reshape(())
        outs[7] = outs[7].T
        return tuple(outs)

    return jax.shard_map(
        shards,
        mesh=mesh,
        in_specs=(P("dp", None, "tm"), P("dp", "tm", None), P(), P(), P(), P(), P(), P()),
        out_specs=(
            P("dp", None, "tm"),
            P("dp", None, "tm"),
            P(),
            P(None, None, "dp", "tm"),
            P(None, "dp", "tm"),
            P(None, "dp", "tm"),
            P(),
            P(),
            P(),
        ),
        check_vma=False,
    )
```
